32 devices in a mesh: dp: 8 (over y, x, core), view: 4 (over z).
Axes of the slice: x: 2, y: 2, z: 4, core: 2. Of those that a mesh axis runs over, the one named last changes fastest.
Arguments:
- pixels: bfloat16 [64, 196, 768], P('dp'), may hold values from -6 to 6
- patch_masks: int32 [64, 4, 196], P('dp'), may hold values from 0 to 1, as said below
- teacher_wide: bfloat16 [768, 6912], P('dp'), may hold values from -0.21875 to 0.21875
- teacher_fc2: bfloat16 [3072, 768], P('dp'), may hold values from -0.109375 to 0.109375
- teacher_vec: bfloat16 [20, 768], P(None, 'dp')
- student_wide: float32 [768, 7680], P('dp'), may hold values from -0.21875 to 0.21875
- student_fc2: float32 [3072, 768], P('dp'), may hold values from -0.109375 to 0.109375
- student_vec: float32 [20, 768], P(None, 'dp')
- wide_first: float32 [768, 7680], P('dp'), may hold values from -9.536743e-07 to 9.536743e-07
- wide_second: float32 [768, 7680], P('dp'), may hold values from 9.670133e-16 to 1.5472212e-14
- fc2_first: float32 [3072, 768], P('dp'), may hold values from -9.536743e-07 to 9.536743e-07
- fc2_second: float32 [3072, 768], P('dp'), may hold values from 9.670133e-16 to 1.5472212e-14
- vec_first: float32 [20, 768], P(None, 'dp'), may hold values from -1.9073486e-05 to 1.9073486e-05
- vec_second: float32 [20, 768], P(None, 'dp'), may hold values from 3.868053e-13 to 6.188885e-12
- step_count: int32 [1], replicated, may hold values from 2 to 20
Outputs:
- loss: float32 [1], replicated
- clip_norm: float32 [1], replicated
- new_wide: float32 [768, 7680], P('dp')
- wide_first_out: float32 [768, 7680], P('dp')
- wide_second_out: float32 [768, 7680], P('dp')
- new_fc2: float32 [3072, 768], P('dp')
- fc2_first_out: float32 [3072, 768], P('dp')
- fc2_second_out: float32 [3072, 768], P('dp')
- new_vec: float32 [20, 768], P(None, 'dp')
- vec_first_out: float32 [20, 768], P(None, 'dp')
- vec_second_out: float32 [20, 768], P(None, 'dp')
The draws below stay inside these ranges and needn't reach their ends.
Inputs may be any that keep to these rules, and one draw needn't show every extreme that they name: `patch_masks`: each view masks between 99 and 137 of the 196 patches, counts drawn independently for each view (they may coincide); in every aligned block of 8 images one image has exactly 137 masked patches in each of its 4 views.
All inputs are finite; a program needn't handle non-finite values.
Results may differ from the reference program's by a relative error of at most 0.0003.
The reference program's roundings to bfloat16 on the way count: a program that leaves them out, or rounds other values in their place, can miss the bound.
Values may be sent and summed in bfloat16 or wider, within the bound.
A program may use at most 256 MiB of HBM per device.

```python
import math
import jax
import jax.numpy as jnp
from jax import lax

D = 768
HEADS = 12
FF = 3072
NP = 196
MMIN = 99
MMAX = 137
VIEWS = 4
GROUP_IMAGES = 8
IMAGES = 64
NVEC = 20
SW = 7680
TW = 6912


def draw_patch_masks(key, part):
    key_count, key_pick, key_perm = jax.random.split(key, 3)
    counts = jax.random.randint(key_count, (IMAGES, VIEWS), MMIN, MMAX + 1)
    groups = IMAGES // GROUP_IMAGES
    chosen = jax.random.randint(key_pick, (groups,), 0, GROUP_IMAGES)
    image_pos = jnp.arange(IMAGES) % GROUP_IMAGES
    full_image = image_pos == jnp.repeat(chosen, GROUP_IMAGES)
    counts = jnp.where(full_image[:, None], MMAX, counts)
    perm_keys = jax.random.split(key_perm, IMAGES * VIEWS)
    rank_table = jax.vmap(lambda sub_key: jax.random.permutation(sub_key, NP))(perm_keys)
    rank_table = rank_table.reshape(IMAGES, VIEWS, NP)
    return (rank_table < counts[:, :, None]).astype(jnp.int32)


def vector_table(key):
    row_index = jnp.arange(NVEC)[:, None]
    gain_rows = (row_index == 3) | (row_index == 8) | (row_index == 9) | (row_index == 12) | (row_index == 13)
    token_rows = row_index <= 1
    normal_draw = jax.random.normal(key, (NVEC, D), jnp.float32)
    return jnp.where(gain_rows, 1.0 + 0.15 * normal_draw, jnp.where(token_rows, normal_draw, 0.3 * normal_draw))


def draw_teacher_vec(key, part):
    return vector_table(jax.random.fold_in(key, 11)).astype(jnp.bfloat16)


def draw_student_vec(key, part):
    return vector_table(jax.random.fold_in(key, 12))


def shard_levels(stream_key, extent, cuts, smallest, top_value):
    gain, own = 1.0, jax.random.fold_in(stream_key, 6)
    for dim, parts in cuts:
        heights = jnp.exp(jax.random.uniform(jax.random.fold_in(own, dim), (parts,), jnp.float32, smallest / len(cuts), top_value / len(cuts)))
        gain = gain * jnp.repeat(heights, extent[dim] // parts).reshape([-1 if axis == dim else 1 for axis in range(len(extent))])
    return gain


def scatter_about(own_key, dims, deviation, bound, cuts=(), kind=jnp.bfloat16):
    level = shard_levels(own_key, dims, cuts, -0.22, 0.18) if cuts else 1.0
    values = jax.random.normal(own_key, dims, jnp.float32) * deviation * level
    return jnp.minimum(jnp.maximum(values, -bound), bound).astype(kind)


def setup_inputs(seed: int = 0) -> dict:
    key_of = jax.random.split(jax.random.key(seed), 16)
    return {
        "pixels": scatter_about(key_of[0], (IMAGES, NP, D), 1.0, 6.0, ((0, 8),)),
        "patch_masks": draw_patch_masks(jax.random.fold_in(key_of[15], 71), 0),
        "teacher_wide": scatter_about(key_of[2], (D, TW), D ** -0.5, 0.21875, ((0, 8),)),
        "teacher_fc2": scatter_about(key_of[3], (FF, D), FF ** -0.5, 0.109375, ((0, 8),)),
        "teacher_vec": draw_teacher_vec(jax.random.fold_in(key_of[15], 71), 0),
        "student_wide": scatter_about(key_of[5], (D, SW), D ** -0.5, 0.21875, ((0, 8),), jnp.float32),
        "student_fc2": scatter_about(key_of[6], (FF, D), FF ** -0.5, 0.109375, ((0, 8),), jnp.float32),
        "student_vec": draw_student_vec(jax.random.fold_in(key_of[15], 71), 0),
        "wide_first": scatter_about(key_of[8], (D, SW), (0.111 * (0.004 ** 2 / (D * SW + FF * D + NVEC * D)) ** 0.5), 9.5367431640625e-07, ((0, 8),), jnp.float32),
        "wide_second": jnp.clip(jnp.exp(math.log(1.547221213453985e-14) - 2.7725887 * jax.random.uniform(key_of[9], (D, SW), jnp.float32) ** shard_levels(key_of[9], (D, SW), ((0, 8),), -0.2, 0.2)), 9.670132584087407e-16, 1.547221213453985e-14),
        "fc2_first": scatter_about(key_of[10], (FF, D), (0.111 * (0.004 ** 2 / (D * SW + FF * D + NVEC * D)) ** 0.5), 9.5367431640625e-07, ((0, 8),), jnp.float32),
        "fc2_second": jnp.clip(jnp.exp(math.log(1.547221213453985e-14) - 2.7725887 * jax.random.uniform(key_of[11], (FF, D), jnp.float32) ** shard_levels(key_of[11], (FF, D), ((0, 8),), -0.2, 0.2)), 9.670132584087407e-16, 1.547221213453985e-14),
        "vec_first": scatter_about(key_of[12], (NVEC, D), (2.22 * (0.004 ** 2 / (D * SW + FF * D + NVEC * D)) ** 0.5), 1.9073486328125e-05, ((1, 8),), jnp.float32),
        "vec_second": jnp.clip(jnp.exp(math.log(6.188884908026049e-12) - 2.7725887 * jax.random.uniform(key_of[13], (NVEC, D), jnp.float32) ** shard_levels(key_of[13], (NVEC, D), ((1, 8),), -0.2, 0.2)), 3.8680530675162805e-13, 6.188884908026049e-12),
        "step_count": jax.random.randint(key_of[14], (1,), 2, 21).astype(jnp.int32),
    }


@jax.custom_vjp
def low(v):
    return lax.optimization_barrier(v.astype(jnp.bfloat16)).astype(jnp.float32)

@jax.custom_vjp
def low_back(v):
    return v

def low_keep(v):
    return (low(v), None)

def low_pass(kept, grad):
    return (grad,)

def back_keep(v):
    return (v, None)

def back_low(kept, grad):
    return (low(grad),)
low.defvjp(low_keep, low_pass)
low_back.defvjp(back_keep, back_low)
precise = lax.Precision.HIGHEST
norm_eps = 1e-06
target_eps = 1e-05
smooth_beta = 2.0
clip_limit = 0.004
beta_one = 0.9
beta_two = 0.999
adam_eps = 1e-08
rate_matrix = 0.03
rate_vector = 0.2
decay_matrix = 0.05

def product(pattern, left_side, right_side):
    return jnp.einsum(pattern, left_side, right_side, precision=precise)

def position_table(length, model_width):
    places = jnp.arange(length).astype(jnp.float32)[:, None]
    freq_index = jnp.arange(model_width // 2).astype(jnp.float32)[None, :]
    angles = places * jnp.exp(freq_index * (-2.0 * math.log(10000.0) / model_width))
    return jnp.stack([jnp.sin(angles), jnp.cos(angles)], axis=-1).reshape(length, model_width)

def layer_norm(values, gain_row, shift_row):
    center = values - lax.optimization_barrier(jnp.mean(values, axis=-1, keepdims=True))
    return center * lax.rsqrt(lax.optimization_barrier(jnp.mean(center * center, axis=-1, keepdims=True)) + norm_eps) * gain_row + shift_row

def embed_rows(patch_vals, weights, vectors, chosen):
    base = low_back(product('bpc,cd->bpd', patch_vals, weights[:, :D]) + vectors[2])
    table = position_table(NP + 1, D)
    patch_rows = jnp.where(chosen[..., None] == 1, vectors[1], base) + table[1:]
    lead = jnp.broadcast_to(vectors[0] + table[0], (patch_rows.shape[0], 1, D))
    return jnp.concatenate([lead, patch_rows], axis=1)

def block_layer(values, weights, second, vectors):
    batch_size, length, model_width = values.shape
    head_dim = model_width // HEADS
    hidden = low(layer_norm(values, vectors[3], vectors[4]))
    bias_qkv = jnp.concatenate([vectors[5], jnp.zeros_like(vectors[5]), vectors[6]])
    packed = low_back(low(product('bsd,de->bse', hidden, weights[:, D:4 * D]) + bias_qkv))
    packed = packed.reshape(batch_size, length, 3, HEADS, head_dim)
    scores = low_back(product('bqhd,bkhd->bhqk', packed[:, :, 0], packed[:, :, 1]) * head_dim ** (-0.5))
    soft_rounded = low(jax.nn.softmax(scores, axis=-1))
    attended = low_back(low(product('bhqk,bkhd->bqhd', soft_rounded, packed[:, :, 2])))
    attended = attended.reshape(batch_size, length, model_width)
    branch = low_back(product('bsd,de->bse', attended, weights[:, 4 * D:5 * D]) + vectors[7])
    middle = values + vectors[8] * branch
    hidden_two = low(layer_norm(middle, vectors[9], vectors[10]))
    pre_act = low_back(product('bsd,df->bsf', hidden_two, weights[:, 5 * D:5 * D + FF]) + vectors[16:].reshape(FF))
    activated = low(jax.nn.gelu(pre_act, approximate=False))
    mlp_out = low_back(product('bsf,fd->bsd', activated, second) + vectors[11])
    return middle + vectors[12] * mlp_out

def slot_list(chosen):
    slot_order = jnp.argsort(1 - chosen, axis=-1, stable=True)[:, :MMAX]
    slot_live = (jnp.arange(MMAX)[None, :] < lax.optimization_barrier(jnp.sum(chosen, axis=-1, keepdims=True))).astype(jnp.float32)
    return (slot_order, slot_live)

def block_loss(copies, pix_block, mask_block, target_block):
    wide, second, vectors = copies
    view_pixels = jnp.repeat(pix_block, VIEWS, axis=0)
    view_masks = mask_block.reshape(GROUP_IMAGES * VIEWS, NP)
    start = embed_rows(view_pixels, wide, vectors, view_masks)
    finished = block_layer(start, wide, second, vectors)
    slot_order, slot_live = slot_list(view_masks)
    picked = jnp.take_along_axis(finished[:, 1:, :], slot_order[:, :, None], axis=1)
    final_rows = low_back(low(layer_norm(picked, vectors[13], vectors[14])))
    predicted = low_back(product('bmd,de->bme', final_rows, wide[:, 5 * D + FF:]) + vectors[15])
    goal = jnp.take_along_axis(jnp.repeat(target_block, VIEWS, axis=0), slot_order[:, :, None], axis=1)
    gap = predicted - goal
    magnitude = jnp.abs(gap)
    terms = jnp.where(magnitude < smooth_beta, 0.5 * gap * gap / smooth_beta, magnitude - 0.5 * smooth_beta)
    return jnp.sum(terms * slot_live[:, :, None])

def adam_step(grad_in, first, second, master, rate, decay, bias_one, bias_two):
    first_new = beta_one * first + (1.0 - beta_one) * grad_in
    second_new = beta_two * second + (1.0 - beta_two) * grad_in * grad_in
    ratio = first_new / bias_one / (jnp.sqrt(second_new / bias_two) + adam_eps)
    return (master - rate * (ratio + decay * master), first_new, second_new)

def reference(pixels, patch_masks, teacher_wide, teacher_fc2, teacher_vec, student_wide, student_fc2, student_vec, wide_first, wide_second, fc2_first, fc2_second, vec_first, vec_second, step_count):
    block_count = IMAGES // GROUP_IMAGES
    pix_blocks = pixels.astype(jnp.float32).reshape(block_count, GROUP_IMAGES, NP, D)
    mask_blocks = patch_masks.reshape(block_count, GROUP_IMAGES, VIEWS, NP)
    t_wide = teacher_wide.astype(jnp.float32)
    t_second = teacher_fc2.astype(jnp.float32)
    t_vectors = teacher_vec.astype(jnp.float32)

    def teacher_block(running, pix_block):
        start = embed_rows(pix_block, t_wide, t_vectors, jnp.zeros((GROUP_IMAGES, NP), jnp.int32))
        patch_out = block_layer(start, t_wide, t_second, t_vectors)[:, 1:, :]
        centered = patch_out - lax.optimization_barrier(jnp.mean(patch_out, axis=1, keepdims=True))
        normed = centered * lax.rsqrt(lax.optimization_barrier(jnp.mean(centered * centered, axis=1, keepdims=True)) + target_eps)
        return (running, low(normed))
    _, targets = lax.scan(teacher_block, jnp.zeros((), jnp.float32), pix_blocks)
    masked_total = jnp.sum(patch_masks).astype(jnp.float32)
    divisor = masked_total * math.sqrt(D)

    def full_loss(params_in):
        copies = tuple((low(item) for item in params_in))
        checked = jax.checkpoint(block_loss)

        def accumulate(running, block_in):
            return (running + checked(copies, block_in[0], block_in[1], block_in[2]), None)
        summed, _ = lax.scan(accumulate, jnp.zeros((), jnp.float32), (pix_blocks, mask_blocks, targets))
        return summed / divisor
    loss_value, pullback = jax.vjp(full_loss, (student_wide, student_fc2, student_vec))
    grads = pullback(jnp.ones((), jnp.float32))[0]
    grad_norm = jnp.sqrt(sum((jnp.sum(item * item) for item in grads)))
    factor = jnp.minimum(1.0, clip_limit / grad_norm)
    steps_done = step_count[0].astype(jnp.float32)
    bias_one = 1.0 - jnp.power(beta_one, steps_done)
    bias_two = 1.0 - jnp.power(beta_two, steps_done)
    new_wide, wide_first_out, wide_second_out = adam_step(grads[0] * factor, wide_first, wide_second, student_wide, rate_matrix, decay_matrix, bias_one, bias_two)
    new_fc2, fc2_first_out, fc2_second_out = adam_step(grads[1] * factor, fc2_first, fc2_second, student_fc2, rate_matrix, decay_matrix, bias_one, bias_two)
    new_vec, vec_first_out, vec_second_out = adam_step(grads[2] * factor, vec_first, vec_second, student_vec, rate_vector, 0.0, bias_one, bias_two)
    return (loss_value.reshape(1), grad_norm.reshape(1), new_wide, wide_first_out, wide_second_out, new_fc2, fc2_first_out, fc2_second_out, new_vec, vec_first_out, vec_second_out)
```

```python
import functools
import math

import jax
import jax.numpy as jnp
from jax import lax
from jax.experimental import pallas as pl
from jax.experimental.pallas import tpu as pltpu
from jax.sharding import PartitionSpec as P

D = 768
HEADS = 12
FF = 3072
NP = 196
ROWS = 208
PAIR = 2
HEAD_SCALE = (D // HEADS) ** (-0.5)

norm_eps = 1e-06
target_eps = 1e-05
smooth_beta = 2.0
clip_limit = 0.004
beta_one = 0.9
beta_two = 0.999
adam_eps = 1e-08
rate_matrix = 0.03
rate_vector = 0.2
decay_matrix = 0.05

f32 = jnp.float32
bf16 = jnp.bfloat16
VMEM_BYTES = 66 * 1024 * 1024 - 2 * 1024 * 1024 - 65536


def dot_nn(a, b):
    return jnp.dot(a, b, preferred_element_type=f32)


def dot_nt(a, b):
    return lax.dot_general(a, b, (((1,), (1,)), ((), ())), preferred_element_type=f32)


def dot_tn(a, b):
    return lax.dot_general(a, b, (((0,), (0,)), ((), ())), preferred_element_type=f32)


def position_table(length, model_width):
    places = jnp.arange(length).astype(f32)[:, None]
    freq_index = jnp.arange(model_width // 2).astype(f32)[None, :]
    angles = places * jnp.exp(freq_index * (-2.0 * math.log(10000.0) / model_width))
    return jnp.stack([jnp.sin(angles), jnp.cos(angles)], axis=-1).reshape(length, model_width)


def normed(values):
    center = values - jnp.mean(values, axis=-1, keepdims=True)
    inverse = lax.rsqrt(jnp.mean(center * center, axis=-1, keepdims=True) + norm_eps)
    return center * inverse, inverse


def norm_back(scaled, unit, inverse):
    return inverse * (
        scaled
        - jnp.mean(scaled, axis=-1, keepdims=True)
        - unit * jnp.mean(scaled * unit, axis=-1, keepdims=True)
    )


def col_sum(values):
    return jnp.sum(values, axis=0, keepdims=True)


def forward_kernel(teacher, *refs):
    if teacher:
        (pix, tab, vec, b1, wide_hbm, w2_hbm, tgt, e, qkv, o, g, wide, w2, sems) = refs
    else:
        (pix, msk, tab, vec, b1, wide_hbm, w2_hbm, e, h, qkv, lse, o, a, h2, gp, g, f, wide, w2, sems) = refs
    cuts = (0, D, 4 * D, 5 * D, 5 * D + FF)
    first = pl.program_id(0) == 0
    copies = [
        pltpu.make_async_copy(
            wide_hbm.at[:, pl.ds(cuts[i], cuts[i + 1] - cuts[i])],
            wide.at[:, pl.ds(cuts[i], cuts[i + 1] - cuts[i])],
            sems.at[i],
        )
        for i in range(4)
    ] + [pltpu.make_async_copy(w2_hbm, w2, sems.at[4])]

    def await_copy(i):
        @pl.when(first)
        def _():
            copies[i].wait()

    @pl.when(first)
    def _():
        for item in copies:
            item.start()

    def row(i):
        return vec[i : i + 1, :]

    await_copy(0)
    for j in range(PAIR):
        base = dot_nn(pix[j], wide[:, :D]) + row(2)
        if not teacher:
            base = jnp.where(msk[j, :NP, :] > 0.5, row(1), base)
        sub = lax.broadcasted_iota(jnp.int32, (16, D), 0)
        e[j, ROWS - 16 :, :] = jnp.where(sub == NP - (ROWS - 16), row(0) + tab[NP : NP + 1, :], 0.0)
        e[j, :NP, :] = base + tab[:NP, :]
    start = e[...].reshape(PAIR * ROWS, D)
    unit, _ = normed(start)
    hidden = (unit * row(3) + row(4)).astype(bf16)
    if not teacher:
        h[...] = hidden.reshape(PAIR, ROWS, D)
    await_copy(1)
    for part, bias in enumerate((5, None, 6)):
        val = dot_nn(hidden, wide[:, D * (part + 1) : D * (part + 2)])
        if bias is not None:
            val = val + row(bias)
        qkv[:, :, D * part : D * (part + 1)] = val.astype(bf16).reshape(PAIR, ROWS, D)

    lane = lax.broadcasted_iota(jnp.int32, (ROWS, 128), 1)
    low_half = lane < 64
    key_bias = jnp.where(lax.broadcasted_iota(jnp.int32, (1, ROWS), 1) <= NP, 0.0, -1e30)

    def attend(j, carry):
        logs = jnp.zeros((ROWS, 128), f32)
        for p in range(HEADS // 2):
            q2 = qkv[j, :, 128 * p : 128 * (p + 1)]
            k2 = qkv[j, :, D + 128 * p : D + 128 * (p + 1)]
            v2 = qkv[j, :, 2 * D + 128 * p : 2 * D + 128 * (p + 1)]
            outs = []
            for half in range(2):
                q_one = jnp.where(low_half if half == 0 else ~low_half, q2, jnp.zeros_like(q2))
                s = dot_nt(q_one, k2) * HEAD_SCALE + key_bias
                peak = jnp.max(s, axis=-1, keepdims=True)
                raised = jnp.exp(s - peak)
                total = jnp.sum(raised, axis=-1, keepdims=True)
                outs.append(dot_nn((raised / total).astype(bf16), v2))
                if not teacher:
                    logs = jnp.where(lane == 2 * p + half, peak + jnp.log(total), logs)
            o[j, :, 128 * p : 128 * (p + 1)] = jnp.where(low_half, outs[0], outs[1]).astype(bf16)
        if not teacher:
            lse[j] = logs
        return carry

    lax.fori_loop(0, PAIR, attend, 0)
    await_copy(2)
    branch = dot_nn(o[...].reshape(PAIR * ROWS, D), wide[:, 4 * D : 5 * D]) + row(7)
    if not teacher:
        a[...] = branch.reshape(PAIR, ROWS, D)
    middle = e[...].reshape(PAIR * ROWS, D) + row(8) * branch
    unit, _ = normed(middle)
    hidden_two = (unit * row(9) + row(10)).astype(bf16)
    if teacher:
        e[...] = middle.reshape(PAIR, ROWS, D)
    else:
        h2[...] = hidden_two.reshape(PAIR, ROWS, D)
    await_copy(3)
    tile = 1024
    for t in range(FF // tile):
        cols = slice(t * tile, (t + 1) * tile)
        pre = dot_nn(hidden_two, wide[:, 5 * D + t * tile : 5 * D + (t + 1) * tile]) + b1[:, cols]
        cumulative = 0.5 * (1.0 + lax.erf(pre * 2.0 ** (-0.5)))
        g[:, :, cols] = (pre * cumulative).astype(bf16).reshape(PAIR, ROWS, tile)
        if not teacher:
            density = jnp.exp(-0.5 * pre * pre) * (2.0 * math.pi) ** (-0.5)
            gp[:, :, cols] = (cumulative + pre * density).reshape(PAIR, ROWS, tile)
    await_copy(4)
    mlp = dot_nn(g[...].reshape(PAIR * ROWS, FF), w2[...]) + row(11)
    if not teacher:
        f[...] = mlp.reshape(PAIR, ROWS, D)
        return
    final = (e[...].reshape(PAIR * ROWS, D) + row(12) * mlp).reshape(PAIR, ROWS, D)
    e[...] = final
    for j in range(PAIR):
        patch = e[j, :NP, :]
        center = patch - jnp.mean(patch, axis=0, keepdims=True)
        tgt[j, ROWS - 16 :, :] = jnp.zeros((16, D), bf16)
        tgt[j, :NP, :] = (
            center * lax.rsqrt(jnp.mean(center * center, axis=0, keepdims=True) + target_eps)
        ).astype(bf16)


def whole(shape):
    return pl.BlockSpec(shape, lambda i: (0,) * len(shape))


def pairs(rows, cols):
    return pl.BlockSpec((PAIR, rows, cols), lambda i: (i, 0, 0))


ANY = pl.BlockSpec(memory_space=pl.ANY)


def params():
    return pltpu.CompilerParams(vmem_limit_bytes=VMEM_BYTES)


def forward(teacher, pixels, mask, table, vectors, wide, second):
    count = pixels.shape[0]
    b1 = vectors[16:].reshape(1, FF)
    cost = pl.CostEstimate(
        flops=int(2 * count * ROWS * (10 * D * D + 2 * D * FF) * (PAIR * 0 + 1)),
        bytes_accessed=60_000_000 if not teacher else 20_000_000,
        transcendentals=count * ROWS * FF * 2,
    )
    scratch_weights = [
        pltpu.VMEM((D, 5 * D + FF), bf16),
        pltpu.VMEM((FF, D), bf16),
        pltpu.SemaphoreType.DMA((5,)),
    ]
    if teacher:
        return pl.pallas_call(
            functools.partial(forward_kernel, True),
            grid=(count // PAIR,),
            in_specs=[pairs(NP, D), whole((ROWS, D)), whole((20, D)), whole((1, FF)), ANY, ANY],
            out_specs=pairs(ROWS, D),
            out_shape=jax.ShapeDtypeStruct((count, ROWS, D), bf16),
            scratch_shapes=[
                pltpu.VMEM((PAIR, ROWS, D), f32),
                pltpu.VMEM((PAIR, ROWS, 3 * D), bf16),
                pltpu.VMEM((PAIR, ROWS, D), bf16),
                pltpu.VMEM((PAIR, ROWS, FF), bf16),
            ]
            + scratch_weights,
            compiler_params=params(),
            cost_estimate=cost,
            name="teacher_forward",
        )(pixels, table, vectors, b1, wide, second)
    kinds = (
        (D, f32),
        (D, bf16),
        (3 * D, bf16),
        (128, f32),
        (D, bf16),
        (D, f32),
        (D, bf16),
        (FF, f32),
        (FF, bf16),
        (D, f32),
    )
    return pl.pallas_call(
        functools.partial(forward_kernel, False),
        grid=(count // PAIR,),
        in_specs=[pairs(NP, D), pairs(ROWS, 1), whole((ROWS, D)), whole((20, D)), whole((1, FF)), ANY, ANY],
        out_specs=[pairs(ROWS, cols) for cols, _ in kinds],
        out_shape=[jax.ShapeDtypeStruct((count, ROWS, cols), kind) for cols, kind in kinds],
        scratch_shapes=scratch_weights,
        compiler_params=params(),
        cost_estimate=cost,
        name="student_forward",
    )(pixels, mask, table, vectors, b1, wide, second)


def back_mlp_kernel(
    div, e, a, f, tgt, msk, gp, vec, wide_hbm, w2_hbm,
    y, dpred, df, du, dx1, acc, accb, wide, w2, sems,
):
    first = pl.program_id(0) == 0
    copies = [
        pltpu.make_async_copy(wide_hbm.at[:, pl.ds(5 * D + FF, D)], wide.at[:, pl.ds(FF, D)], sems.at[0]),
        pltpu.make_async_copy(w2_hbm, w2, sems.at[1]),
        pltpu.make_async_copy(wide_hbm.at[:, pl.ds(5 * D, FF)], wide.at[:, pl.ds(0, FF)], sems.at[2]),
    ]

    def await_copy(i):
        @pl.when(first)
        def _():
            copies[i].wait()

    @pl.when(first)
    def _():
        for item in copies:
            item.start()
        acc[...] = jnp.zeros_like(acc)
        accb[...] = jnp.zeros_like(accb)

    def row(i):
        return vec[i : i + 1, :]

    def add(i, val):
        acc[i : i + 1, :] += val

    count = PAIR * ROWS
    middle = e[...].reshape(count, D) + row(8) * a[...].reshape(count, D)
    mlp = f[...].reshape(count, D)
    unit, inverse = normed(middle + row(12) * mlp)
    rows_in = (unit * row(13) + row(14)).astype(bf16)
    y[...] = rows_in.reshape(PAIR, ROWS, D)
    await_copy(0)
    gap = dot_nn(rows_in, wide[:, FF:]) + row(15) - tgt[...].reshape(count, D).astype(f32)
    live = msk[...].reshape(count, 1) > 0.5
    size = jnp.abs(gap)
    terms = jnp.where(size < smooth_beta, 0.5 * gap * gap / smooth_beta, size - 0.5 * smooth_beta)
    add(0, col_sum(jnp.where(live, terms, 0.0)))
    slope = jnp.where(live, jnp.clip(gap / smooth_beta, -1.0, 1.0) / div[0, 0], 0.0).astype(bf16)
    dpred[...] = slope.reshape(PAIR, ROWS, D)
    add(15, col_sum(slope.astype(f32)))
    dy = dot_nt(slope, wide[:, FF:]).astype(bf16).astype(f32)
    add(13, col_sum(dy * unit))
    add(14, col_sum(dy))
    dx2 = norm_back(dy * row(13), unit, inverse)
    add(12, col_sum(mlp * dx2))
    dmlp = (row(12) * dx2).astype(bf16)
    df[...] = dmlp.reshape(PAIR, ROWS, D)
    add(11, col_sum(dmlp.astype(f32)))
    dx1[...] = dx2.reshape(PAIR, ROWS, D)
    await_copy(1)
    tile = 1024
    for t in range(FF // tile):
        cols = slice(t * tile, (t + 1) * tile)
        val = dot_nt(dmlp, w2[cols, :]) * gp[:, :, cols].reshape(count, tile)
        val = val.astype(bf16)
        du[:, :, cols] = val.reshape(PAIR, ROWS, tile)
        accb[:, cols] += col_sum(val.astype(f32))
    await_copy(2)
    dh2 = dot_nt(du[...].reshape(count, FF), wide[:, :FF])
    middle = e[...].reshape(count, D) + row(8) * a[...].reshape(count, D)
    unit, inverse = normed(middle)
    add(9, col_sum(dh2 * unit))
    add(10, col_sum(dh2))
    grad = dx1[...].reshape(count, D) + norm_back(dh2 * row(9), unit, inverse)
    dx1[...] = grad.reshape(PAIR, ROWS, D)


def back_mlp(divisor, e, a, f, targets, mask, gp, vectors, wide, second):
    count = e.shape[0]
    kinds = ((D, bf16), (D, bf16), (D, bf16), (FF, bf16), (D, f32))
    return pl.pallas_call(
        back_mlp_kernel,
        grid=(count // PAIR,),
        in_specs=[
            pl.BlockSpec(memory_space=pltpu.SMEM),
            pairs(ROWS, D), pairs(ROWS, D), pairs(ROWS, D), pairs(ROWS, D), pairs(ROWS, 1), pairs(ROWS, FF),
            whole((20, D)), ANY, ANY,
        ],
        out_specs=[pairs(ROWS, cols) for cols, _ in kinds] + [whole((16, D)), whole((1, FF))],
        out_shape=[jax.ShapeDtypeStruct((count, ROWS, cols), kind) for cols, kind in kinds]
        + [jax.ShapeDtypeStruct((16, D), f32), jax.ShapeDtypeStruct((1, FF), f32)],
        scratch_shapes=[
            pltpu.VMEM((D, FF + D), bf16),
            pltpu.VMEM((FF, D), bf16),
            pltpu.SemaphoreType.DMA((3,)),
        ],
        compiler_params=params(),
        cost_estimate=pl.CostEstimate(
            flops=2 * count * ROWS * (2 * D * D + 2 * D * FF), bytes_accessed=70_000_000, transcendentals=0
        ),
        name="back_mlp",
    )(divisor, e, a, f, targets, mask, gp, vectors, wide, second)


def back_attention_kernel(
    dx1, a, e, qkv, lse, msk, vec, wide_hbm, da, dqkv, dbase, acc, d_att, wide, sems
):
    first = pl.program_id(0) == 0
    copies = [
        pltpu.make_async_copy(wide_hbm.at[:, pl.ds(4 * D, D)], wide.at[:, pl.ds(3 * D, D)], sems.at[0]),
        pltpu.make_async_copy(wide_hbm.at[:, pl.ds(D, 3 * D)], wide.at[:, pl.ds(0, 3 * D)], sems.at[1]),
    ]

    def await_copy(i):
        @pl.when(first)
        def _():
            copies[i].wait()

    @pl.when(first)
    def _():
        for item in copies:
            item.start()
        acc[...] = jnp.zeros_like(acc)

    def row(i):
        return vec[i : i + 1, :]

    def add(i, val):
        acc[i : i + 1, :] += val

    count = PAIR * ROWS
    grad = dx1[...].reshape(count, D)
    add(8, col_sum(a[...].reshape(count, D) * grad))
    dbranch = (row(8) * grad).astype(bf16)
    da[...] = dbranch.reshape(PAIR, ROWS, D)
    add(7, col_sum(dbranch.astype(f32)))
    await_copy(0)
    d_att[...] = dot_nt(dbranch, wide[:, 3 * D :]).astype(bf16).reshape(PAIR, ROWS, D)

    lane = lax.broadcasted_iota(jnp.int32, (ROWS, 128), 1)
    low_half = lane < 64
    key_live = lax.broadcasted_iota(jnp.int32, (1, ROWS), 1) <= NP

    def attend(j, carry):
        for p in range(HEADS // 2):
            cols = slice(128 * p, 128 * (p + 1))
            q2 = qkv[j, :, 128 * p : 128 * (p + 1)]
            k2 = qkv[j, :, D + 128 * p : D + 128 * (p + 1)]
            v2 = qkv[j, :, 2 * D + 128 * p : 2 * D + 128 * (p + 1)]
            do2 = d_att[j, :, cols]
            dq, dk, dv = [], [], []
            for half in range(2):
                pick = low_half if half == 0 else ~low_half
                zero = jnp.zeros_like(q2)
                s = dot_nt(jnp.where(pick, q2, zero), k2) * HEAD_SCALE
                soft = jnp.where(key_live, jnp.exp(s - lse[j, :, 2 * p + half : 2 * p + half + 1]), 0.0)
                dsoft = dot_nt(jnp.where(pick, do2, zero), v2)
                dv.append(dot_tn(soft.astype(bf16), do2))
                dscore = soft * (dsoft - jnp.sum(dsoft * soft, axis=-1, keepdims=True))
                dscore = dscore.astype(bf16)
                dq.append(dot_nn(dscore, k2))
                dk.append(dot_tn(dscore, q2))
            dqkv[j, :, 128 * p : 128 * (p + 1)] = (jnp.where(low_half, dq[0], dq[1]) * HEAD_SCALE).astype(bf16)
            dqkv[j, :, D + 128 * p : D + 128 * (p + 1)] = (
                jnp.where(low_half, dk[0], dk[1]) * HEAD_SCALE
            ).astype(bf16)
            dqkv[j, :, 2 * D + 128 * p : 2 * D + 128 * (p + 1)] = jnp.where(low_half, dv[0], dv[1]).astype(bf16)
        return carry

    lax.fori_loop(0, PAIR, attend, 0)
    add(5, col_sum(dqkv[:, :, :D].reshape(count, D).astype(f32)))
    add(6, col_sum(dqkv[:, :, 2 * D :].reshape(count, D).astype(f32)))
    await_copy(1)
    dh = dot_nt(dqkv[...].reshape(count, 3 * D), wide[:, : 3 * D])
    unit, inverse = normed(e[...].reshape(count, D))
    add(3, col_sum(dh * unit))
    add(4, col_sum(dh))
    d_start = dx1[...].reshape(count, D) + norm_back(dh * row(3), unit, inverse)
    place = lax.broadcasted_iota(jnp.int32, (PAIR, ROWS, 1), 1).reshape(count, 1)
    hit = msk[...].reshape(count, 1) > 0.5
    add(0, col_sum(jnp.where(place == NP, d_start, 0.0)))
    add(1, col_sum(jnp.where(hit, d_start, 0.0)))
    kept = jnp.where(hit | (place >= NP), 0.0, d_start).astype(bf16)
    add(2, col_sum(kept.astype(f32)))
    kept = kept.reshape(PAIR, ROWS, D)
    for j in range(PAIR):
        dbase[j] = kept[j, :NP, :]


def back_attention(dx1, a, e, qkv, lse, mask, vectors, wide):
    count = e.shape[0]
    return pl.pallas_call(
        back_attention_kernel,
        grid=(count // PAIR,),
        in_specs=[
            pairs(ROWS, D), pairs(ROWS, D), pairs(ROWS, D), pairs(ROWS, 3 * D), pairs(ROWS, 128), pairs(ROWS, 1),
            whole((20, D)), ANY,
        ],
        out_specs=[pairs(ROWS, D), pairs(ROWS, 3 * D), pairs(NP, D), whole((16, D))],
        out_shape=[
            jax.ShapeDtypeStruct((count, ROWS, D), bf16),
            jax.ShapeDtypeStruct((count, ROWS, 3 * D), bf16),
            jax.ShapeDtypeStruct((count, NP, D), bf16),
            jax.ShapeDtypeStruct((16, D), f32),
        ],
        scratch_shapes=[
            pltpu.VMEM((PAIR, ROWS, D), bf16),
            pltpu.VMEM((D, 4 * D), bf16),
            pltpu.SemaphoreType.DMA((2,)),
        ],
        compiler_params=params(),
        cost_estimate=pl.CostEstimate(
            flops=2 * count * ROWS * (4 * D * D + 10 * ROWS * D), bytes_accessed=40_000_000, transcendentals=0
        ),
        name="back_attention",
    )(dx1, a, e, qkv, lse, mask, vectors, wide)


def weight_grad(rows_in, grads):
    return jnp.einsum("bsd,bse->de", rows_in, grads, preferred_element_type=f32)


def adam_step(grad_in, first, second, master, rate, decay, bias_one, bias_two):
    first_new = beta_one * first + (1.0 - beta_one) * grad_in
    second_new = beta_two * second + (1.0 - beta_two) * grad_in * grad_in
    ratio = first_new / bias_one / (jnp.sqrt(second_new / bias_two) + adam_eps)
    return (master - rate * (ratio + decay * master), first_new, second_new)


def update_all(grad_list, first_list, second_list, master_list, factor, bias_one, bias_two):
    rates = (rate_matrix, rate_matrix, rate_vector)
    decays = (decay_matrix, decay_matrix, 0.0)
    results = []
    for index in range(3):
        results.extend(
            adam_step(
                grad_list[index] * factor,
                first_list[index],
                second_list[index],
                master_list[index],
                rates[index],
                decays[index],
                bias_one,
                bias_two,
            )
        )
    return results


def square_total(grad_list):
    return sum(jnp.sum(item * item) for item in grad_list)


def body(
    pixels,
    patch_masks,
    teacher_wide,
    teacher_fc2,
    teacher_vec,
    student_wide,
    student_fc2,
    student_vec,
    wide_first,
    wide_second,
    fc2_first,
    fc2_second,
    vec_first,
    vec_second,
    step_count,
):
    view_id = lax.axis_index("view")
    view_count = lax.axis_size("view")
    group_size = pixels.shape[0]
    owned_images = group_size // view_count
    t_wide, t_second, t_vec, s_wide, s_second, s_vec = (
        lax.all_gather(teacher_wide, "dp", axis=0, tiled=True),
        lax.all_gather(teacher_fc2, "dp", axis=0, tiled=True),
        lax.all_gather(teacher_vec, "dp", axis=1, tiled=True),
        lax.all_gather(student_wide.astype(bf16), "dp", axis=0, tiled=True),
        lax.all_gather(student_fc2.astype(bf16), "dp", axis=0, tiled=True),
        lax.all_gather(student_vec.astype(bf16), "dp", axis=1, tiled=True),
    )
    t_vectors = t_vec.astype(f32)
    s_vectors = s_vec.astype(f32)
    masked_total = lax.psum(jnp.sum(patch_masks).astype(f32), "dp")
    divisor = masked_total * math.sqrt(D)
    places = position_table(NP + 1, D)
    table = jnp.concatenate([places[1:], places[:1], jnp.zeros((ROWS - NP - 1, D), f32)], axis=0)
    own_pixels = lax.dynamic_slice_in_dim(pixels, view_id * owned_images, owned_images, 0)
    own_targets = forward(True, own_pixels, None, table, t_vectors, t_wide, t_second)
    targets = lax.all_gather(own_targets, "view", axis=0, tiled=True)
    my_masks = lax.dynamic_index_in_dim(patch_masks, view_id, 1, keepdims=False)
    mask = jnp.pad(my_masks.astype(f32), ((0, 0), (0, ROWS - NP)))[:, :, None]
    e, h, qkv, lse, o, a, h2, gp, g, f = forward(
        False, pixels, mask, table, s_vectors, s_wide, s_second
    )
    y, dpred, df, du, dx1, acc_mlp, acc_b1 = back_mlp(
        divisor.reshape(1, 1), e, a, f, targets, mask, gp, s_vectors, s_wide, s_second
    )
    g_head = weight_grad(y, dpred)
    g_second = weight_grad(g, df)
    g_first = weight_grad(h2, du)
    da, dqkv, dbase, acc_att = back_attention(dx1, a, e, qkv, lse, mask, s_vectors, s_wide)
    g_proj = weight_grad(o, da)
    g_qkv = weight_grad(h, dqkv)
    g_patch = weight_grad(pixels, dbase)
    loss_part = jnp.sum(acc_mlp[0])
    g_wide = jnp.concatenate([g_patch, g_qkv, g_proj, g_first, g_head], axis=1)
    g_vec = jnp.concatenate([acc_att[:9], acc_mlp[9:], acc_b1.reshape(-1, D)], axis=0)
    steps_done = step_count[0].astype(f32)
    bias_one = 1.0 - jnp.power(beta_one, steps_done)
    bias_two = 1.0 - jnp.power(beta_two, steps_done)
    shard_wide, shard_second, shard_vec = (
        lax.psum_scatter(g_wide, "dp", scatter_dimension=0, tiled=True),
        lax.psum_scatter(g_second, "dp", scatter_dimension=0, tiled=True),
        lax.psum_scatter(g_vec, "dp", scatter_dimension=1, tiled=True),
    )
    shard_wide, shard_second, shard_vec, loss_view = lax.psum(
        (shard_wide, shard_second, shard_vec, loss_part), "view"
    )
    grad_list = (shard_wide, shard_second, shard_vec)
    square_all, loss_all = lax.psum((square_total(grad_list), loss_view), "dp")
    grad_norm = jnp.sqrt(square_all)
    factor = jnp.minimum(1.0, clip_limit / grad_norm)
    results = update_all(
        grad_list,
        (wide_first, fc2_first, vec_first),
        (wide_second, fc2_second, vec_second),
        (student_wide, student_fc2, student_vec),
        factor,
        bias_one,
        bias_two,
    )
    return ((loss_all / divisor).reshape(1), grad_norm.reshape(1), *results)


def solution(mesh):
    in_specs = (
        P("dp", None, None),
        P("dp", None, None),
        P("dp", None),
        P("dp", None),
        P(None, "dp"),
        P("dp", None),
        P("dp", None),
        P(None, "dp"),
        P("dp", None),
        P("dp", None),
        P("dp", None),
        P("dp", None),
        P(None, "dp"),
        P(None, "dp"),
        P(),
    )
    out_specs = (
        P(),
        P(),
        P("dp", None),
        P("dp", None),
        P("dp", None),
        P("dp", None),
        P("dp", None),
        P("dp", None),
        P(None, "dp"),
        P(None, "dp"),
        P(None, "dp"),
    )
    return jax.shard_map(body, mesh=mesh, in_specs=in_specs, out_specs=out_specs, check_vma=False)
```

```python
import functools
import math

import jax
import jax.numpy as jnp
from jax import lax
from jax.experimental import pallas as pl
from jax.experimental.pallas import tpu as pltpu
from jax.sharding import PartitionSpec as P

D = 768
HEADS = 12
FF = 3072
NP = 196
ROWS = 208
PAIR = 2
HEAD_SCALE = (D // HEADS) ** (-0.5)

norm_eps = 1e-06
target_eps = 1e-05
smooth_beta = 2.0
clip_limit = 0.004
beta_one = 0.9
beta_two = 0.999
adam_eps = 1e-08
rate_matrix = 0.03
rate_vector = 0.2
decay_matrix = 0.05

f32 = jnp.float32
bf16 = jnp.bfloat16
VMEM_BYTES = 66 * 1024 * 1024 - 2 * 1024 * 1024 - 65536


def dot_nn(a, b):
    return jnp.dot(a, b, preferred_element_type=f32)


def dot_nt(a, b):
    return lax.dot_general(a, b, (((1,), (1,)), ((), ())), preferred_element_type=f32)


def dot_tn(a, b):
    return lax.dot_general(a, b, (((0,), (0,)), ((), ())), preferred_element_type=f32)


def position_table(length, model_width):
    places = jnp.arange(length).astype(f32)[:, None]
    freq_index = jnp.arange(model_width // 2).astype(f32)[None, :]
    angles = places * jnp.exp(freq_index * (-2.0 * math.log(10000.0) / model_width))
    return jnp.stack([jnp.sin(angles), jnp.cos(angles)], axis=-1).reshape(length, model_width)


def normed(values):
    center = values - jnp.mean(values, axis=-1, keepdims=True)
    inverse = lax.rsqrt(jnp.mean(center * center, axis=-1, keepdims=True) + norm_eps)
    return center * inverse, inverse


def norm_back(scaled, unit, inverse):
    return inverse * (
        scaled
        - jnp.mean(scaled, axis=-1, keepdims=True)
        - unit * jnp.mean(scaled * unit, axis=-1, keepdims=True)
    )


def col_sum(values):
    return jnp.sum(values, axis=0, keepdims=True)


def forward_kernel(teacher, *refs):
    if teacher:
        (pix, tab, vec, b1, wide_hbm, w2_hbm, tgt, e, qkv, o, g, wide, w2, sems) = refs
    else:
        (pix, msk, tab, vec, b1, wide_hbm, w2_hbm, e, h, qkv, lse, o, a, h2, gp, g, f, wide, w2, sems) = refs
    cuts = (0, D, 4 * D, 5 * D, 5 * D + FF)
    first = pl.program_id(0) == 0
    copies = [
        pltpu.make_async_copy(
            wide_hbm.at[:, pl.ds(cuts[i], cuts[i + 1] - cuts[i])],
            wide.at[:, pl.ds(cuts[i], cuts[i + 1] - cuts[i])],
            sems.at[i],
        )
        for i in range(4)
    ] + [pltpu.make_async_copy(w2_hbm, w2, sems.at[4])]

    def await_copy(i):
        @pl.when(first)
        def _():
            copies[i].wait()

    @pl.when(first)
    def _():
        for item in copies:
            item.start()

    def row(i):
        return vec[i : i + 1, :]

    await_copy(0)
    for j in range(PAIR):
        base = dot_nn(pix[j], wide[:, :D]) + row(2)
        if not teacher:
            base = jnp.where(msk[j, :NP, :] > 0.5, row(1), base)
        sub = lax.broadcasted_iota(jnp.int32, (16, D), 0)
        e[j, ROWS - 16 :, :] = jnp.where(sub == NP - (ROWS - 16), row(0) + tab[NP : NP + 1, :], 0.0)
        e[j, :NP, :] = base + tab[:NP, :]
    start = e[...].reshape(PAIR * ROWS, D)
    unit, _ = normed(start)
    hidden = (unit * row(3) + row(4)).astype(bf16)
    if not teacher:
        h[...] = hidden.reshape(PAIR, ROWS, D)
    await_copy(1)
    for part, bias in enumerate((5, None, 6)):
        val = dot_nn(hidden, wide[:, D * (part + 1) : D * (part + 2)])
        if bias is not None:
            val = val + row(bias)
        qkv[:, :, D * part : D * (part + 1)] = val.astype(bf16).reshape(PAIR, ROWS, D)

    lane = lax.broadcasted_iota(jnp.int32, (ROWS, 128), 1)
    low_half = lane < 64
    key_bias = jnp.where(lax.broadcasted_iota(jnp.int32, (1, ROWS), 1) <= NP, 0.0, -1e30)

    def attend(j, carry):
        logs = jnp.zeros((ROWS, 128), f32)
        for p in range(HEADS // 2):
            q2 = qkv[j, :, 128 * p : 128 * (p + 1)]
            k2 = qkv[j, :, D + 128 * p : D + 128 * (p + 1)]
            v2 = qkv[j, :, 2 * D + 128 * p : 2 * D + 128 * (p + 1)]
            outs = []
            for half in range(2):
                q_one = jnp.where(low_half if half == 0 else ~low_half, q2, jnp.zeros_like(q2))
                s = dot_nt(q_one, k2) * HEAD_SCALE + key_bias
                peak = jnp.max(s, axis=-1, keepdims=True)
                raised = jnp.exp(s - peak)
                total = jnp.sum(raised, axis=-1, keepdims=True)
                outs.append(dot_nn((raised / total).astype(bf16), v2))
                if not teacher:
                    logs = jnp.where(lane == 2 * p + half, peak + jnp.log(total), logs)
            o[j, :, 128 * p : 128 * (p + 1)] = jnp.where(low_half, outs[0], outs[1]).astype(bf16)
        if not teacher:
            lse[j] = logs
        return carry

    lax.fori_loop(0, PAIR, attend, 0)
    await_copy(2)
    branch = dot_nn(o[...].reshape(PAIR * ROWS, D), wide[:, 4 * D : 5 * D]) + row(7)
    if not teacher:
        a[...] = branch.reshape(PAIR, ROWS, D)
    middle = e[...].reshape(PAIR * ROWS, D) + row(8) * branch
    unit, _ = normed(middle)
    hidden_two = (unit * row(9) + row(10)).astype(bf16)
    if teacher:
        e[...] = middle.reshape(PAIR, ROWS, D)
    else:
        h2[...] = hidden_two.reshape(PAIR, ROWS, D)
    await_copy(3)
    tile = 1024
    for t in range(FF // tile):
        cols = slice(t * tile, (t + 1) * tile)
        pre = dot_nn(hidden_two, wide[:, 5 * D + t * tile : 5 * D + (t + 1) * tile]) + b1[:, cols]
        cumulative = 0.5 * (1.0 + lax.erf(pre * 2.0 ** (-0.5)))
        g[:, :, cols] = (pre * cumulative).astype(bf16).reshape(PAIR, ROWS, tile)
        if not teacher:
            density = jnp.exp(-0.5 * pre * pre) * (2.0 * math.pi) ** (-0.5)
            gp[:, :, cols] = (cumulative + pre * density).reshape(PAIR, ROWS, tile)
    await_copy(4)
    mlp = dot_nn(g[...].reshape(PAIR * ROWS, FF), w2[...]) + row(11)
    if not teacher:
        f[...] = mlp.reshape(PAIR, ROWS, D)
        return
    final = (e[...].reshape(PAIR * ROWS, D) + row(12) * mlp).reshape(PAIR, ROWS, D)
    e[...] = final
    for j in range(PAIR):
        patch = e[j, :NP, :]
        center = patch - jnp.mean(patch, axis=0, keepdims=True)
        tgt[j, ROWS - 16 :, :] = jnp.zeros((16, D), bf16)
        tgt[j, :NP, :] = (
            center * lax.rsqrt(jnp.mean(center * center, axis=0, keepdims=True) + target_eps)
        ).astype(bf16)


def whole(shape):
    return pl.BlockSpec(shape, lambda i: (0,) * len(shape))


def pairs(rows, cols):
    return pl.BlockSpec((PAIR, rows, cols), lambda i: (i, 0, 0))


ANY = pl.BlockSpec(memory_space=pl.ANY)


def params():
    return pltpu.CompilerParams(vmem_limit_bytes=VMEM_BYTES)


def forward(teacher, pixels, mask, table, vectors, wide, second):
    count = pixels.shape[0]
    b1 = vectors[16:].reshape(1, FF)
    cost = pl.CostEstimate(
        flops=int(2 * count * ROWS * (10 * D * D + 2 * D * FF) * (PAIR * 0 + 1)),
        bytes_accessed=60_000_000 if not teacher else 20_000_000,
        transcendentals=count * ROWS * FF * 2,
    )
    scratch_weights = [
        pltpu.VMEM((D, 5 * D + FF), bf16),
        pltpu.VMEM((FF, D), bf16),
        pltpu.SemaphoreType.DMA((5,)),
    ]
    if teacher:
        return pl.pallas_call(
            functools.partial(forward_kernel, True),
            grid=(count // PAIR,),
            in_specs=[pairs(NP, D), whole((ROWS, D)), whole((20, D)), whole((1, FF)), ANY, ANY],
            out_specs=pairs(ROWS, D),
            out_shape=jax.ShapeDtypeStruct((count, ROWS, D), bf16),
            scratch_shapes=[
                pltpu.VMEM((PAIR, ROWS, D), f32),
                pltpu.VMEM((PAIR, ROWS, 3 * D), bf16),
                pltpu.VMEM((PAIR, ROWS, D), bf16),
                pltpu.VMEM((PAIR, ROWS, FF), bf16),
            ]
            + scratch_weights,
            compiler_params=params(),
            cost_estimate=cost,
            name="teacher_forward",
        )(pixels, table, vectors, b1, wide, second)
    kinds = (
        (D, f32),
        (D, bf16),
        (3 * D, bf16),
        (128, f32),
        (D, bf16),
        (D, f32),
        (D, bf16),
        (FF, f32),
        (FF, bf16),
        (D, f32),
    )
    return pl.pallas_call(
        functools.partial(forward_kernel, False),
        grid=(count // PAIR,),
        in_specs=[pairs(NP, D), pairs(ROWS, 1), whole((ROWS, D)), whole((20, D)), whole((1, FF)), ANY, ANY],
        out_specs=[pairs(ROWS, cols) for cols, _ in kinds],
        out_shape=[jax.ShapeDtypeStruct((count, ROWS, cols), kind) for cols, kind in kinds],
        scratch_shapes=scratch_weights,
        compiler_params=params(),
        cost_estimate=cost,
        name="student_forward",
    )(pixels, mask, table, vectors, b1, wide, second)


def back_mlp_kernel(
    div, e, a, f, tgt, msk, gp, vec, wide_hbm, w2_hbm,
    y, dpred, df, du, dx1, acc, accb, wide, w2, sems,
):
    first = pl.program_id(0) == 0
    copies = [
        pltpu.make_async_copy(wide_hbm.at[:, pl.ds(5 * D + FF, D)], wide.at[:, pl.ds(FF, D)], sems.at[0]),
        pltpu.make_async_copy(w2_hbm, w2, sems.at[1]),
        pltpu.make_async_copy(wide_hbm.at[:, pl.ds(5 * D, FF)], wide.at[:, pl.ds(0, FF)], sems.at[2]),
    ]

    def await_copy(i):
        @pl.when(first)
        def _():
            copies[i].wait()

    @pl.when(first)
    def _():
        for item in copies:
            item.start()
        acc[...] = jnp.zeros_like(acc)
        accb[...] = jnp.zeros_like(accb)

    def row(i):
        return vec[i : i + 1, :]

    def add(i, val):
        acc[i : i + 1, :] += val

    count = PAIR * ROWS
    middle = e[...].reshape(count, D) + row(8) * a[...].reshape(count, D)
    mlp = f[...].reshape(count, D)
    unit, inverse = normed(middle + row(12) * mlp)
    rows_in = (unit * row(13) + row(14)).astype(bf16)
    y[...] = rows_in.reshape(PAIR, ROWS, D)
    await_copy(0)
    gap = dot_nn(rows_in, wide[:, FF:]) + row(15) - tgt[...].reshape(count, D).astype(f32)
    live = msk[...].reshape(count, 1) > 0.5
    size = jnp.abs(gap)
    terms = jnp.where(size < smooth_beta, 0.5 * gap * gap / smooth_beta, size - 0.5 * smooth_beta)
    add(0, col_sum(jnp.where(live, terms, 0.0)))
    slope = jnp.where(live, jnp.clip(gap / smooth_beta, -1.0, 1.0) / div[0, 0], 0.0).astype(bf16)
    dpred[...] = slope.reshape(PAIR, ROWS, D)
    add(15, col_sum(slope.astype(f32)))
    dy = dot_nt(slope, wide[:, FF:]).astype(bf16).astype(f32)
    add(13, col_sum(dy * unit))
    add(14, col_sum(dy))
    dx2 = norm_back(dy * row(13), unit, inverse)
    add(12, col_sum(mlp * dx2))
    dmlp = (row(12) * dx2).astype(bf16)
    df[...] = dmlp.reshape(PAIR, ROWS, D)
    add(11, col_sum(dmlp.astype(f32)))
    dx1[...] = dx2.reshape(PAIR, ROWS, D)
    await_copy(1)
    tile = 1024
    for t in range(FF // tile):
        cols = slice(t * tile, (t + 1) * tile)
        val = dot_nt(dmlp, w2[cols, :]) * gp[:, :, cols].reshape(count, tile)
        val = val.astype(bf16)
        du[:, :, cols] = val.reshape(PAIR, ROWS, tile)
        accb[:, cols] += col_sum(val.astype(f32))
    await_copy(2)
    dh2 = dot_nt(du[...].reshape(count, FF), wide[:, :FF])
    middle = e[...].reshape(count, D) + row(8) * a[...].reshape(count, D)
    unit, inverse = normed(middle)
    add(9, col_sum(dh2 * unit))
    add(10, col_sum(dh2))
    grad = dx1[...].reshape(count, D) + norm_back(dh2 * row(9), unit, inverse)
    dx1[...] = grad.reshape(PAIR, ROWS, D)


def back_mlp(divisor, e, a, f, targets, mask, gp, vectors, wide, second):
    count = e.shape[0]
    kinds = ((D, bf16), (D, bf16), (D, bf16), (FF, bf16), (D, f32))
    return pl.pallas_call(
        back_mlp_kernel,
        grid=(count // PAIR,),
        in_specs=[
            pl.BlockSpec(memory_space=pltpu.SMEM),
            pairs(ROWS, D), pairs(ROWS, D), pairs(ROWS, D), pairs(ROWS, D), pairs(ROWS, 1), pairs(ROWS, FF),
            whole((20, D)), ANY, ANY,
        ],
        out_specs=[pairs(ROWS, cols) for cols, _ in kinds] + [whole((16, D)), whole((1, FF))],
        out_shape=[jax.ShapeDtypeStruct((count, ROWS, cols), kind) for cols, kind in kinds]
        + [jax.ShapeDtypeStruct((16, D), f32), jax.ShapeDtypeStruct((1, FF), f32)],
        scratch_shapes=[
            pltpu.VMEM((D, FF + D), bf16),
            pltpu.VMEM((FF, D), bf16),
            pltpu.SemaphoreType.DMA((3,)),
        ],
        compiler_params=params(),
        cost_estimate=pl.CostEstimate(
            flops=2 * count * ROWS * (2 * D * D + 2 * D * FF), bytes_accessed=70_000_000, transcendentals=0
        ),
        name="back_mlp",
    )(divisor, e, a, f, targets, mask, gp, vectors, wide, second)


def back_attention_kernel(
    dx1, a, e, qkv, lse, msk, vec, wide_hbm, da, dqkv, dbase, acc, d_att, wide, sems
):
    first = pl.program_id(0) == 0
    copies = [
        pltpu.make_async_copy(wide_hbm.at[:, pl.ds(4 * D, D)], wide.at[:, pl.ds(3 * D, D)], sems.at[0]),
        pltpu.make_async_copy(wide_hbm.at[:, pl.ds(D, 3 * D)], wide.at[:, pl.ds(0, 3 * D)], sems.at[1]),
    ]

    def await_copy(i):
        @pl.when(first)
        def _():
            copies[i].wait()

    @pl.when(first)
    def _():
        for item in copies:
            item.start()
        acc[...] = jnp.zeros_like(acc)

    def row(i):
        return vec[i : i + 1, :]

    def add(i, val):
        acc[i : i + 1, :] += val

    count = PAIR * ROWS
    grad = dx1[...].reshape(count, D)
    add(8, col_sum(a[...].reshape(count, D) * grad))
    dbranch = (row(8) * grad).astype(bf16)
    da[...] = dbranch.reshape(PAIR, ROWS, D)
    add(7, col_sum(dbranch.astype(f32)))
    await_copy(0)
    d_att[...] = dot_nt(dbranch, wide[:, 3 * D :]).astype(bf16).reshape(PAIR, ROWS, D)

    lane = lax.broadcasted_iota(jnp.int32, (ROWS, 128), 1)
    low_half = lane < 64
    key_live = lax.broadcasted_iota(jnp.int32, (1, ROWS), 1) <= NP

    def attend(j, carry):
        for p in range(HEADS // 2):
            cols = slice(128 * p, 128 * (p + 1))
            q2 = qkv[j, :, 128 * p : 128 * (p + 1)]
            k2 = qkv[j, :, D + 128 * p : D + 128 * (p + 1)]
            v2 = qkv[j, :, 2 * D + 128 * p : 2 * D + 128 * (p + 1)]
            do2 = d_att[j, :, cols]
            dq, dk, dv = [], [], []
            for half in range(2):
                pick = low_half if half == 0 else ~low_half
                zero = jnp.zeros_like(q2)
                s = dot_nt(jnp.where(pick, q2, zero), k2) * HEAD_SCALE
                soft = jnp.where(key_live, jnp.exp(s - lse[j, :, 2 * p + half : 2 * p + half + 1]), 0.0)
                dsoft = dot_nt(jnp.where(pick, do2, zero), v2)
                dv.append(dot_tn(soft.astype(bf16), do2))
                dscore = soft * (dsoft - jnp.sum(dsoft * soft, axis=-1, keepdims=True))
                dscore = dscore.astype(bf16)
                dq.append(dot_nn(dscore, k2))
                dk.append(dot_tn(dscore, q2))
            dqkv[j, :, 128 * p : 128 * (p + 1)] = (jnp.where(low_half, dq[0], dq[1]) * HEAD_SCALE).astype(bf16)
            dqkv[j, :, D + 128 * p : D + 128 * (p + 1)] = (
                jnp.where(low_half, dk[0], dk[1]) * HEAD_SCALE
            ).astype(bf16)
            dqkv[j, :, 2 * D + 128 * p : 2 * D + 128 * (p + 1)] = jnp.where(low_half, dv[0], dv[1]).astype(bf16)
        return carry

    lax.fori_loop(0, PAIR, attend, 0)
    add(5, col_sum(dqkv[:, :, :D].reshape(count, D).astype(f32)))
    add(6, col_sum(dqkv[:, :, 2 * D :].reshape(count, D).astype(f32)))
    await_copy(1)
    dh = dot_nt(dqkv[...].reshape(count, 3 * D), wide[:, : 3 * D])
    unit, inverse = normed(e[...].reshape(count, D))
    add(3, col_sum(dh * unit))
    add(4, col_sum(dh))
    d_start = dx1[...].reshape(count, D) + norm_back(dh * row(3), unit, inverse)
    place = lax.broadcasted_iota(jnp.int32, (PAIR, ROWS, 1), 1).reshape(count, 1)
    hit = msk[...].reshape(count, 1) > 0.5
    add(0, col_sum(jnp.where(place == NP, d_start, 0.0)))
    add(1, col_sum(jnp.where(hit, d_start, 0.0)))
    kept = jnp.where(hit | (place >= NP), 0.0, d_start).astype(bf16)
    add(2, col_sum(kept.astype(f32)))
    kept = kept.reshape(PAIR, ROWS, D)
    for j in range(PAIR):
        dbase[j] = kept[j, :NP, :]


def back_attention(dx1, a, e, qkv, lse, mask, vectors, wide):
    count = e.shape[0]
    return pl.pallas_call(
        back_attention_kernel,
        grid=(count // PAIR,),
        in_specs=[
            pairs(ROWS, D), pairs(ROWS, D), pairs(ROWS, D), pairs(ROWS, 3 * D), pairs(ROWS, 128), pairs(ROWS, 1),
            whole((20, D)), ANY,
        ],
        out_specs=[pairs(ROWS, D), pairs(ROWS, 3 * D), pairs(NP, D), whole((16, D))],
        out_shape=[
            jax.ShapeDtypeStruct((count, ROWS, D), bf16),
            jax.ShapeDtypeStruct((count, ROWS, 3 * D), bf16),
            jax.ShapeDtypeStruct((count, NP, D), bf16),
            jax.ShapeDtypeStruct((16, D), f32),
        ],
        scratch_shapes=[
            pltpu.VMEM((PAIR, ROWS, D), bf16),
            pltpu.VMEM((D, 4 * D), bf16),
            pltpu.SemaphoreType.DMA((2,)),
        ],
        compiler_params=params(),
        cost_estimate=pl.CostEstimate(
            flops=2 * count * ROWS * (4 * D * D + 10 * ROWS * D), bytes_accessed=40_000_000, transcendentals=0
        ),
        name="back_attention",
    )(dx1, a, e, qkv, lse, mask, vectors, wide)


def weight_grad(rows_in, grads):
    return jnp.einsum("bsd,bse->de", rows_in, grads, preferred_element_type=f32)
CHUNK = 256
SLOTS = 8
AHEAD = 2
LAG = 2
MESH = pl.DeviceIdType.MESH


def bit_orders(m):
    left = list(range(m - 1, -1, -1))
    return left, left[m // 2 :] + left[: m // 2]


def reduce_kernel(m, n_wide, n_fc, rows, wide_in, fc_in, wide_out, fc_out, norm_out, *scratch):
    stage_in = scratch[3 : 3 + m]
    work, core_in, acc = scratch[:3]
    za, zb, nbuf = scratch[3 + m : 6 + m]
    (load_s, core_s, core_r, half_s, half_r, z1_s, z1_r, z2_s, z2_r, z3_s, z3_r, out_s, n_s, n_r) = scratch[6 + m :]
    count = n_wide + n_fc
    fc_cols = D // CHUNK
    half = CHUNK // 2
    dp, z = lax.axis_index("dp"), lax.axis_index("view")
    core = dp % 2
    own = [(dp // (2 ** (m - d))) % 2 for d in range(m)]
    partner = (dp + 1 - 2 * core, z)
    peers = [(dp + (1 - 2 * own[d]) * 2 ** (m - d), z) for d in range(m)]
    outer = (z == 0) | (z == 3)
    inner = (z == 1) | (z == 2)
    to_inner = (dp, 1 + z // 3)
    to_outer = (dp, (z - 1) * 3)
    across = (dp, 3 - z)
    orders = bit_orders(m)
    full = (slice(None),) * m

    barrier = pltpu.get_barrier_semaphore()
    for peer in [partner] + peers:
        pl.semaphore_signal(barrier, inc=1, device_id=peer, device_id_type=MESH)

    @pl.when(outer)
    def _():
        pl.semaphore_signal(barrier, inc=1, device_id=to_inner, device_id_type=MESH)
        pl.semaphore_wait(barrier, m + 2)

    @pl.when(inner)
    def _():
        pl.semaphore_signal(barrier, inc=1, device_id=to_outer, device_id_type=MESH)
        pl.semaphore_signal(barrier, inc=1, device_id=across, device_id_type=MESH)
        pl.semaphore_wait(barrier, m + 3)

    def remote(src, dst, send, recv, device):
        return pltpu.make_async_remote_copy(
            src_ref=src, dst_ref=dst, send_sem=send, recv_sem=recv, device_id=device, device_id_type=MESH
        )

    def slot(k):
        return lax.rem(k, SLOTS)

    def guarded(k, step):
        @pl.when((k >= 0) & (k < count))
        def _():
            step(k)

    def source(k, which, act):
        @pl.when(k < n_wide)
        def _():
            act(wide_in.at[full + (which, slice(None), pl.ds(pl.multiple_of(k * CHUNK, CHUNK), CHUNK))])

        @pl.when(k >= n_wide)
        def _():
            q = k - n_wide
            act(
                fc_in.at[
                    full
                    + (
                        which,
                        pl.ds(pl.multiple_of((q // fc_cols) * rows, 8), rows),
                        pl.ds(pl.multiple_of((q % fc_cols) * CHUNK, CHUNK), CHUNK),
                    )
                ]
            )

    def begin(k):
        s = slot(k)
        source(k, 1 - core, lambda ref: remote(ref, core_in.at[k], core_s.at[s], core_r.at[s], partner).start())
        source(k, core, lambda ref: pltpu.make_async_copy(ref, work.at[k], load_s.at[s]).start())

    def lead(order, stage, flip):
        out = []
        for d in range(m):
            if d in order[:stage]:
                out.append(own[d])
            elif d == order[stage]:
                out.append(1 - own[d] if flip else own[d])
            else:
                out.append(slice(None))
        return tuple(out)

    def exchange(k, stage, side):
        order = orders[side]
        s = slot(k)
        cols = slice(side * half, (side + 1) * half)
        return remote(
            work.at[(k,) + lead(order, stage, True) + (slice(None), cols)],
            stage_in[stage].at[k, side],
            half_s.at[s, stage, side],
            half_r.at[s, stage, side],
            peers[order[stage]],
        )

    def by_rows(body):
        def go(i, carry):
            body(pl.ds(pl.multiple_of(i * 8, 8), 8))
            return carry

        lax.fori_loop(0, rows // 8, go, 0)

    def merge_core(k):
        s = slot(k)
        pltpu.make_async_copy(core_in.at[k], work.at[k], load_s.at[s]).wait()
        remote(work.at[k], core_in.at[k], core_s.at[s], core_r.at[s], partner).wait()

        def body(r):
            at = (k,) + full + (r, slice(None))
            work[at] = work[at] + core_in[at]

        by_rows(body)
        for side in range(2):
            exchange(k, 0, side).start()

    def merge_stage(k, stage):
        for side in range(2):
            exchange(k, stage, side).wait()
            order = orders[side]
            cols = slice(side * half, (side + 1) * half)

            def body(r):
                at = (k,) + lead(order, stage, False) + (r, cols)
                work[at] = work[at] + stage_in[stage][(k, side) + (slice(None),) * (m - stage - 1) + (r, slice(None))]

            by_rows(body)
            if stage + 1 < m:
                exchange(k, stage + 1, side).start()
        if stage + 1 == m:

            @pl.when(outer)
            def _():
                chain_one(k).start()

    def mine(k):
        return work.at[(k,) + tuple(own)]

    def chain_one(k):
        return remote(mine(k), za.at[k], z1_s.at[slot(k)], z1_r.at[slot(k)], to_inner)

    def chain_two(k):
        return remote(mine(k), zb.at[k], z2_s.at[slot(k)], z2_r.at[slot(k)], across)

    def chain_three(k):
        return remote(za.at[k], za.at[k], z3_s.at[slot(k)], z3_r.at[slot(k)], to_outer)

    def meet(k):
        @pl.when(inner)
        def _():
            chain_one(k).wait_recv()

            def body(r):
                at = (k,) + tuple(own) + (r, slice(None))
                work[at] = work[at] + za[k, r, :]

            by_rows(body)
            chain_two(k).start()

    def total(k):
        @pl.when(inner)
        def _():
            chain_two(k).wait()

            def body(r):
                za[k, r, :] = work[(k,) + tuple(own) + (r, slice(None))] + zb[k, r, :]

            by_rows(body)
            chain_three(k).start()

    def target(k, act):
        @pl.when(k < n_wide)
        def _():
            act(wide_out.at[:, pl.ds(pl.multiple_of(k * CHUNK, CHUNK), CHUNK)])

        @pl.when(k >= n_wide)
        def _():
            q = k - n_wide
            act(
                fc_out.at[
                    pl.ds(pl.multiple_of((q // fc_cols) * rows, 8), rows),
                    pl.ds(pl.multiple_of((q % fc_cols) * CHUNK, CHUNK), CHUNK),
                ]
            )

    lanes = lax.broadcasted_iota(jnp.int32, (8, CHUNK), 1)

    def finish(k):
        s = slot(k)

        @pl.when(outer)
        def _():
            chain_one(k).wait_send()
            pltpu.make_async_remote_copy(
                src_ref=za.at[k], dst_ref=za.at[k], send_sem=z3_s.at[s], recv_sem=z3_r.at[s],
                device_id=to_inner, device_id_type=MESH,
            ).wait_recv()

        @pl.when(inner)
        def _():
            chain_three(k).wait_send()

        @pl.when(k >= SLOTS)
        def _():
            pltpu.make_async_copy(za.at[k], za.at[k], out_s.at[s]).wait()

        target(k, lambda ref: pltpu.make_async_copy(za.at[k], ref, out_s.at[s]).start())
        live = (lanes < 20) | (k != n_wide - 1)

        def body(r):
            val = jnp.where(live, za[k, r, :], 0.0)
            acc[...] += val * val

        by_rows(body)

    acc[...] = jnp.zeros_like(acc)
    for k in range(AHEAD):
        begin(jnp.int32(k))

    def step(t, carry):
        guarded(t + AHEAD, begin)
        guarded(t, merge_core)
        for stage in range(m):
            guarded(t - LAG * (stage + 1), functools.partial(merge_stage, stage=stage))
        guarded(t - LAG * (m + 1), meet)
        guarded(t - LAG * (m + 2), total)
        guarded(t - LAG * (m + 3), finish)
        return carry

    lax.fori_loop(0, count + LAG * (m + 3), step, 0)
    for k in range(count - SLOTS, count):
        pltpu.make_async_copy(za.at[k], za.at[k], out_s.at[k % SLOTS]).wait()

    nbuf[0] = acc[:, :128] + acc[:, 128:]
    for j, peer in enumerate([partner] + peers):
        copy = remote(nbuf.at[2 * j], nbuf.at[2 * j + 1], n_s.at[j], n_r.at[j], peer)
        copy.start()
        copy.wait()
        nbuf[2 * j + 2] = nbuf[2 * j] + nbuf[2 * j + 1]
    norm_out[...] = nbuf[2 * m + 2]


def reduce_all(wide, fc2, dp):
    m = dp.bit_length() - 2
    rows = D // dp
    n_wide, n_fc = wide.shape[1] // CHUNK, 4 * D // CHUNK
    count = n_wide + n_fc
    lead = (2,) * m
    sent = count * CHUNK * rows * 4 * 12
    dma = pltpu.SemaphoreType.DMA
    return pl.pallas_call(
        functools.partial(reduce_kernel, m, n_wide, n_fc, rows),
        in_specs=[ANY, ANY],
        out_specs=[ANY, ANY, pl.BlockSpec(memory_space=pltpu.VMEM)],
        out_shape=[
            jax.ShapeDtypeStruct((rows, wide.shape[1]), f32),
            jax.ShapeDtypeStruct((4 * rows, D), f32),
            jax.ShapeDtypeStruct((8, 128), f32),
        ],
        scratch_shapes=[
            pltpu.VMEM((count,) + lead + (rows, CHUNK), f32),
            pltpu.VMEM((count,) + lead + (rows, CHUNK), f32),
            pltpu.VMEM((8, CHUNK), f32),
        ]
        + [pltpu.VMEM((count, 2) + (2,) * (m - s - 1) + (rows, CHUNK // 2), f32) for s in range(m)]
        + [
            pltpu.VMEM((count, rows, CHUNK), f32),
            pltpu.VMEM((count, rows, CHUNK), f32),
            pltpu.VMEM((2 * m + 3, 8, 128), f32),
            dma((SLOTS,)), dma((SLOTS,)), dma((SLOTS,)), dma((SLOTS, m, 2)), dma((SLOTS, m, 2)),
        ]
        + [dma((SLOTS,))] * 7
        + [dma((m + 1,)), dma((m + 1,))],
        compiler_params=pltpu.CompilerParams(
            vmem_limit_bytes=VMEM_BYTES, collective_id=0, has_side_effects=True
        ),
        cost_estimate=pl.CostEstimate(flops=1_000_000, bytes_accessed=66_000_000, transcendentals=0),
        name="reduce_gradients",
    )(
        wide.reshape(lead + (2, rows, wide.shape[1])),
        fc2.reshape(lead + (2, 4 * rows, D)),
    )


def adam_step(grad_in, first, second, master, rate, decay, bias_one, bias_two):
    first_new = beta_one * first + (1.0 - beta_one) * grad_in
    second_new = beta_two * second + (1.0 - beta_two) * grad_in * grad_in
    ratio = first_new / bias_one / (jnp.sqrt(second_new / bias_two) + adam_eps)
    return (master - rate * (ratio + decay * master), first_new, second_new)


def update_all(grad_list, first_list, second_list, master_list, factor, bias_one, bias_two):
    rates = (rate_matrix, rate_matrix, rate_vector)
    decays = (decay_matrix, decay_matrix, 0.0)
    results = []
    for index in range(3):
        results.extend(
            adam_step(
                grad_list[index] * factor,
                first_list[index],
                second_list[index],
                master_list[index],
                rates[index],
                decays[index],
                bias_one,
                bias_two,
            )
        )
    return results


def body(
    pixels,
    patch_masks,
    teacher_wide,
    teacher_fc2,
    teacher_vec,
    student_wide,
    student_fc2,
    student_vec,
    wide_first,
    wide_second,
    fc2_first,
    fc2_second,
    vec_first,
    vec_second,
    step_count,
):
    view_id = lax.axis_index("view")
    view_count = lax.axis_size("view")
    group_size = pixels.shape[0]
    owned_images = group_size // view_count
    t_wide, t_second, t_vec, s_wide, s_second, s_vec = (
        lax.all_gather(teacher_wide, "dp", axis=0, tiled=True),
        lax.all_gather(teacher_fc2, "dp", axis=0, tiled=True),
        lax.all_gather(teacher_vec, "dp", axis=1, tiled=True),
        lax.all_gather(student_wide.astype(bf16), "dp", axis=0, tiled=True),
        lax.all_gather(student_fc2.astype(bf16), "dp", axis=0, tiled=True),
        lax.all_gather(student_vec.astype(bf16), "dp", axis=1, tiled=True),
    )
    t_vectors = t_vec.astype(f32)
    s_vectors = s_vec.astype(f32)
    masked_total = lax.psum(jnp.sum(patch_masks).astype(f32), "dp")
    divisor = masked_total * math.sqrt(D)
    places = position_table(NP + 1, D)
    table = jnp.concatenate([places[1:], places[:1], jnp.zeros((ROWS - NP - 1, D), f32)], axis=0)
    own_pixels = lax.dynamic_slice_in_dim(pixels, view_id * owned_images, owned_images, 0)
    own_targets = forward(True, own_pixels, None, table, t_vectors, t_wide, t_second)
    targets = lax.all_gather(own_targets, "view", axis=0, tiled=True)
    my_masks = lax.dynamic_index_in_dim(patch_masks, view_id, 1, keepdims=False)
    mask = jnp.pad(my_masks.astype(f32), ((0, 0), (0, ROWS - NP)))[:, :, None]
    e, h, qkv, lse, o, a, h2, gp, g, f = forward(
        False, pixels, mask, table, s_vectors, s_wide, s_second
    )
    y, dpred, df, du, dx1, acc_mlp, acc_b1 = back_mlp(
        divisor.reshape(1, 1), e, a, f, targets, mask, gp, s_vectors, s_wide, s_second
    )
    g_head = weight_grad(y, dpred)
    g_second = weight_grad(g, df)
    g_first = weight_grad(h2, du)
    da, dqkv, dbase, acc_att = back_attention(dx1, a, e, qkv, lse, mask, s_vectors, s_wide)
    g_proj = weight_grad(o, da)
    g_qkv = weight_grad(h, dqkv)
    g_patch = weight_grad(pixels, dbase)
    loss_part = jnp.sum(acc_mlp[0])
    g_vec = jnp.concatenate([acc_att[:9], acc_mlp[9:], acc_b1.reshape(-1, D)], axis=0)
    extra = jnp.concatenate([g_vec, jnp.broadcast_to(loss_part, (1, D)), jnp.zeros((CHUNK - 21, D), f32)], axis=0)
    g_wide = jnp.concatenate([g_patch, g_qkv, g_proj, g_first, g_head, extra.T], axis=1)
    steps_done = step_count[0].astype(f32)
    bias_one = 1.0 - jnp.power(beta_one, steps_done)
    bias_two = 1.0 - jnp.power(beta_two, steps_done)
    wide_all, shard_second, squares = reduce_all(g_wide, g_second, lax.axis_size("dp"))
    width = student_wide.shape[1]
    shard_wide, shard_vec = wide_all[:, :width], wide_all[:, width : width + 20].T
    loss_all = wide_all[0, width + 20]
    grad_list = (shard_wide, shard_second, shard_vec)
    grad_norm = jnp.sqrt(jnp.sum(squares))
    factor = jnp.minimum(1.0, clip_limit / grad_norm)
    results = update_all(
        grad_list,
        (wide_first, fc2_first, vec_first),
        (wide_second, fc2_second, vec_second),
        (student_wide, student_fc2, student_vec),
        factor,
        bias_one,
        bias_two,
    )
    return ((loss_all / divisor).reshape(1), grad_norm.reshape(1), *results)


def solution(mesh):
    in_specs = (
        P("dp", None, None),
        P("dp", None, None),
        P("dp", None),
        P("dp", None),
        P(None, "dp"),
        P("dp", None),
        P("dp", None),
        P(None, "dp"),
        P("dp", None),
        P("dp", None),
        P("dp", None),
        P("dp", None),
        P(None, "dp"),
        P(None, "dp"),
        P(),
    )
    out_specs = (
        P(),
        P(),
        P("dp", None),
        P("dp", None),
        P("dp", None),
        P("dp", None),
        P("dp", None),
        P("dp", None),
        P(None, "dp"),
        P(None, "dp"),
        P(None, "dp"),
    )
    return jax.shard_map(body, mesh=mesh, in_specs=in_specs, out_specs=out_specs, check_vma=False)
```

```python
import functools
import math

import jax
import jax.numpy as jnp
from jax import lax
from jax.experimental import pallas as pl
from jax.experimental.pallas import tpu as pltpu
from jax.sharding import PartitionSpec as P

D = 768
HEADS = 12
FF = 3072
NP = 196
ROWS = 208
PAIR = 2
HEAD_SCALE = (D // HEADS) ** (-0.5)

norm_eps = 1e-06
target_eps = 1e-05
smooth_beta = 2.0
clip_limit = 0.004
beta_one = 0.9
beta_two = 0.999
adam_eps = 1e-08
rate_matrix = 0.03
rate_vector = 0.2
decay_matrix = 0.05

f32 = jnp.float32
bf16 = jnp.bfloat16
VMEM_BYTES = 66 * 1024 * 1024 - 2 * 1024 * 1024 - 65536


def dot_nn(a, b):
    return jnp.dot(a, b, preferred_element_type=f32)


def dot_nt(a, b):
    return lax.dot_general(a, b, (((1,), (1,)), ((), ())), preferred_element_type=f32)


def dot_tn(a, b):
    return lax.dot_general(a, b, (((0,), (0,)), ((), ())), preferred_element_type=f32)


def frequencies():
    index = (jnp.arange(D) // 2).astype(f32)
    return jnp.exp(index * (-2.0 * math.log(10000.0) / D)).reshape(1, D)


def normed(values):
    center = values - jnp.mean(values, axis=-1, keepdims=True)
    inverse = lax.rsqrt(jnp.mean(center * center, axis=-1, keepdims=True) + norm_eps)
    return center * inverse, inverse


def norm_back(scaled, unit, inverse):
    return inverse * (
        scaled
        - jnp.mean(scaled, axis=-1, keepdims=True)
        - unit * jnp.mean(scaled * unit, axis=-1, keepdims=True)
    )


def col_sum(values):
    return jnp.sum(values, axis=0, keepdims=True)


def forward_kernel(teacher, *refs):
    if teacher:
        (pix, tab, vec, b1, wide_hbm, w2_hbm, tgt, e, qkv, o, g, wide, w2, sems) = refs
    else:
        (pix, msk, tab, vec, b1, wide_hbm, w2_hbm, e, h, qkv, lse, o, a, h2, gp, g, f, wide, w2, sems) = refs
    cuts = (0, D, 4 * D, 5 * D, 5 * D + FF)
    first = pl.program_id(0) == 0
    copies = [
        pltpu.make_async_copy(
            wide_hbm.at[:, pl.ds(cuts[i], cuts[i + 1] - cuts[i])],
            wide.at[:, pl.ds(cuts[i], cuts[i + 1] - cuts[i])],
            sems.at[i],
        )
        for i in range(4)
    ] + [pltpu.make_async_copy(w2_hbm, w2, sems.at[4])]

    def await_copy(i):
        @pl.when(first)
        def _():
            copies[i].wait()

    @pl.when(first)
    def _():
        for item in copies:
            item.start()

    def row(i):
        return vec[i : i + 1, :]

    await_copy(0)
    for j in range(PAIR):
        if teacher or j == 0:
            patches = dot_nn(pix[j], wide[:, :D]) + row(2)
        base = patches if teacher else jnp.where(msk[j, :NP, :] > 0.5, row(1), patches)
        sub = lax.broadcasted_iota(jnp.int32, (16, D), 0)
        e[j, ROWS - 16 :, :] = jnp.where(sub == NP - (ROWS - 16), row(0) + tab[NP : NP + 1, :], 0.0)
        e[j, :NP, :] = base + tab[:NP, :]
    start = e[...].reshape(PAIR * ROWS, D)
    unit, _ = normed(start)
    hidden = (unit * row(3) + row(4)).astype(bf16)
    if not teacher:
        h[...] = hidden.reshape(PAIR, ROWS, D)
    await_copy(1)
    for part, bias in enumerate((5, None, 6)):
        val = dot_nn(hidden, wide[:, D * (part + 1) : D * (part + 2)])
        if bias is not None:
            val = val + row(bias)
        qkv[:, :, D * part : D * (part + 1)] = val.astype(bf16).reshape(PAIR, ROWS, D)

    lane = lax.broadcasted_iota(jnp.int32, (ROWS, 128), 1)
    low_half = lane < 64
    key_bias = jnp.where(lax.broadcasted_iota(jnp.int32, (1, ROWS), 1) <= NP, 0.0, -1e30)

    def attend(j, carry):
        logs = jnp.zeros((ROWS, 128), f32)
        for p in range(HEADS // 2):
            q2 = qkv[j, :, 128 * p : 128 * (p + 1)]
            k2 = qkv[j, :, D + 128 * p : D + 128 * (p + 1)]
            v2 = qkv[j, :, 2 * D + 128 * p : 2 * D + 128 * (p + 1)]
            outs = []
            for half in range(2):
                q_one = jnp.where(low_half if half == 0 else ~low_half, q2, jnp.zeros_like(q2))
                s = dot_nt(q_one, k2) * HEAD_SCALE + key_bias
                peak = jnp.max(s, axis=-1, keepdims=True)
                raised = jnp.exp(s - peak)
                total = jnp.sum(raised, axis=-1, keepdims=True)
                outs.append(dot_nn((raised / total).astype(bf16), v2))
                if not teacher:
                    logs = jnp.where(lane == 2 * p + half, peak + jnp.log(total), logs)
            o[j, :, 128 * p : 128 * (p + 1)] = jnp.where(low_half, outs[0], outs[1]).astype(bf16)
        if not teacher:
            lse[j] = logs
        return carry

    lax.fori_loop(0, PAIR, attend, 0)
    await_copy(2)
    branch = dot_nn(o[...].reshape(PAIR * ROWS, D), wide[:, 4 * D : 5 * D]) + row(7)
    if not teacher:
        a[...] = branch.reshape(PAIR, ROWS, D)
    middle = e[...].reshape(PAIR * ROWS, D) + row(8) * branch
    unit, _ = normed(middle)
    hidden_two = (unit * row(9) + row(10)).astype(bf16)
    if teacher:
        e[...] = middle.reshape(PAIR, ROWS, D)
    else:
        h2[...] = hidden_two.reshape(PAIR, ROWS, D)
    await_copy(3)
    tile = 1024
    for t in range(FF // tile):
        cols = slice(t * tile, (t + 1) * tile)
        pre = dot_nn(hidden_two, wide[:, 5 * D + t * tile : 5 * D + (t + 1) * tile]) + b1[:, cols]
        cumulative = 0.5 * (1.0 + lax.erf(pre * 2.0 ** (-0.5)))
        g[:, :, cols] = (pre * cumulative).astype(bf16).reshape(PAIR, ROWS, tile)
        if not teacher:
            density = jnp.exp(-0.5 * pre * pre) * (2.0 * math.pi) ** (-0.5)
            gp[:, :, cols] = (cumulative + pre * density).reshape(PAIR, ROWS, tile)
    await_copy(4)
    mlp = dot_nn(g[...].reshape(PAIR * ROWS, FF), w2[...]) + row(11)
    if not teacher:
        f[...] = mlp.reshape(PAIR, ROWS, D)
        return
    final = (e[...].reshape(PAIR * ROWS, D) + row(12) * mlp).reshape(PAIR, ROWS, D)
    e[...] = final
    for j in range(PAIR):
        patch = e[j, :NP, :]
        center = patch - jnp.mean(patch, axis=0, keepdims=True)
        tgt[j, ROWS - 16 :, :] = jnp.zeros((16, D), bf16)
        tgt[j, :NP, :] = (
            center * lax.rsqrt(jnp.mean(center * center, axis=0, keepdims=True) + target_eps)
        ).astype(bf16)


def whole(shape):
    return pl.BlockSpec(shape, lambda i: (0,) * len(shape))


def pairs(rows, cols):
    return pl.BlockSpec((PAIR, rows, cols), lambda i: (i, 0, 0))


ANY = pl.BlockSpec(memory_space=pl.ANY)


def params():
    return pltpu.CompilerParams(vmem_limit_bytes=VMEM_BYTES)


def per_image(rows, cols, pairs_each):
    return pl.BlockSpec((1, rows, cols), lambda i: (i // pairs_each, 0, 0))


def forward(teacher, pixels, mask, table, vectors, wide, second):
    count = pixels.shape[0] if teacher else mask.shape[0]
    pairs_each = max(count // pixels.shape[0] // PAIR, 1)
    b1 = vectors[16:].reshape(1, FF)
    cost = pl.CostEstimate(
        flops=int(2 * count * ROWS * (10 * D * D + 2 * D * FF) * (PAIR * 0 + 1)),
        bytes_accessed=60_000_000 if not teacher else 20_000_000,
        transcendentals=count * ROWS * FF * 2,
    )
    scratch_weights = [
        pltpu.VMEM((D, 5 * D + FF), bf16),
        pltpu.VMEM((FF, D), bf16),
        pltpu.SemaphoreType.DMA((5,)),
    ]
    if teacher:
        return pl.pallas_call(
            functools.partial(forward_kernel, True),
            grid=(count // PAIR,),
            in_specs=[pairs(NP, D), whole((ROWS, D)), whole((20, D)), whole((1, FF)), ANY, ANY],
            out_specs=pairs(ROWS, D),
            out_shape=jax.ShapeDtypeStruct((count, ROWS, D), bf16),
            scratch_shapes=[
                pltpu.VMEM((PAIR, ROWS, D), f32),
                pltpu.VMEM((PAIR, ROWS, 3 * D), bf16),
                pltpu.VMEM((PAIR, ROWS, D), bf16),
                pltpu.VMEM((PAIR, ROWS, FF), bf16),
            ]
            + scratch_weights,
            compiler_params=params(),
            cost_estimate=cost,
            name="teacher_forward",
        )(pixels, table, vectors, b1, wide, second)
    kinds = (
        (D, f32),
        (D, bf16),
        (3 * D, bf16),
        (128, f32),
        (D, bf16),
        (D, f32),
        (D, bf16),
        (FF, f32),
        (FF, bf16),
        (D, f32),
    )
    return pl.pallas_call(
        functools.partial(forward_kernel, False),
        grid=(count // PAIR,),
        in_specs=[
            per_image(NP, D, pairs_each), pairs(ROWS, 1), whole((ROWS, D)), whole((20, D)), whole((1, FF)), ANY, ANY,
        ],
        out_specs=[pairs(ROWS, cols) for cols, _ in kinds],
        out_shape=[jax.ShapeDtypeStruct((count, ROWS, cols), kind) for cols, kind in kinds],
        scratch_shapes=scratch_weights,
        compiler_params=params(),
        cost_estimate=cost,
        name="student_forward",
    )(pixels, mask, table, vectors, b1, wide, second)


def back_mlp_kernel(
    div, e, a, f, tgt, msk, gp, vec, wide_hbm, w2_hbm,
    y, dpred, df, du, dx1, acc, accb, wide, w2, sems,
):
    first = pl.program_id(0) == 0
    copies = [
        pltpu.make_async_copy(wide_hbm.at[:, pl.ds(5 * D + FF, D)], wide.at[:, pl.ds(FF, D)], sems.at[0]),
        pltpu.make_async_copy(w2_hbm, w2, sems.at[1]),
        pltpu.make_async_copy(wide_hbm.at[:, pl.ds(5 * D, FF)], wide.at[:, pl.ds(0, FF)], sems.at[2]),
    ]

    def await_copy(i):
        @pl.when(first)
        def _():
            copies[i].wait()

    @pl.when(first)
    def _():
        for item in copies:
            item.start()
        acc[...] = jnp.zeros_like(acc)
        accb[...] = jnp.zeros_like(accb)

    def row(i):
        return vec[i : i + 1, :]

    def add(i, val):
        acc[i : i + 1, :] += val

    count = PAIR * ROWS
    middle = e[...].reshape(count, D) + row(8) * a[...].reshape(count, D)
    mlp = f[...].reshape(count, D)
    unit, inverse = normed(middle + row(12) * mlp)
    rows_in = (unit * row(13) + row(14)).astype(bf16)
    y[...] = rows_in.reshape(PAIR, ROWS, D)
    await_copy(0)
    goal = jnp.broadcast_to(tgt[...].astype(f32), (PAIR, ROWS, D)).reshape(count, D)
    gap = dot_nn(rows_in, wide[:, FF:]) + row(15) - goal
    live = msk[...].reshape(count, 1) > 0.5
    size = jnp.abs(gap)
    terms = jnp.where(size < smooth_beta, 0.5 * gap * gap / smooth_beta, size - 0.5 * smooth_beta)
    add(0, col_sum(jnp.where(live, terms, 0.0)))
    slope = jnp.where(live, jnp.clip(gap / smooth_beta, -1.0, 1.0) / div[0, 0], 0.0).astype(bf16)
    dpred[...] = slope.reshape(PAIR, ROWS, D)
    add(15, col_sum(slope.astype(f32)))
    dy = dot_nt(slope, wide[:, FF:]).astype(bf16).astype(f32)
    add(13, col_sum(dy * unit))
    add(14, col_sum(dy))
    dx2 = norm_back(dy * row(13), unit, inverse)
    add(12, col_sum(mlp * dx2))
    dmlp = (row(12) * dx2).astype(bf16)
    df[...] = dmlp.reshape(PAIR, ROWS, D)
    add(11, col_sum(dmlp.astype(f32)))
    dx1[...] = dx2.reshape(PAIR, ROWS, D)
    await_copy(1)
    tile = 1024
    for t in range(FF // tile):
        cols = slice(t * tile, (t + 1) * tile)
        val = dot_nt(dmlp, w2[cols, :]) * gp[:, :, cols].reshape(count, tile)
        val = val.astype(bf16)
        du[:, :, cols] = val.reshape(PAIR, ROWS, tile)
        accb[:, cols] += col_sum(val.astype(f32))
    await_copy(2)
    dh2 = dot_nt(du[...].reshape(count, FF), wide[:, :FF])
    middle = e[...].reshape(count, D) + row(8) * a[...].reshape(count, D)
    unit, inverse = normed(middle)
    add(9, col_sum(dh2 * unit))
    add(10, col_sum(dh2))
    grad = dx1[...].reshape(count, D) + norm_back(dh2 * row(9), unit, inverse)
    dx1[...] = grad.reshape(PAIR, ROWS, D)


def back_mlp(divisor, e, a, f, targets, mask, gp, vectors, wide, second):
    count = e.shape[0]
    pairs_each = count // targets.shape[0] // PAIR
    kinds = ((D, bf16), (D, bf16), (D, bf16), (FF, bf16), (D, f32))
    return pl.pallas_call(
        back_mlp_kernel,
        grid=(count // PAIR,),
        in_specs=[
            pl.BlockSpec(memory_space=pltpu.SMEM),
            pairs(ROWS, D), pairs(ROWS, D), pairs(ROWS, D), per_image(ROWS, D, pairs_each), pairs(ROWS, 1),
            pairs(ROWS, FF),
            whole((20, D)), ANY, ANY,
        ],
        out_specs=[pairs(ROWS, cols) for cols, _ in kinds] + [whole((16, D)), whole((1, FF))],
        out_shape=[jax.ShapeDtypeStruct((count, ROWS, cols), kind) for cols, kind in kinds]
        + [jax.ShapeDtypeStruct((16, D), f32), jax.ShapeDtypeStruct((1, FF), f32)],
        scratch_shapes=[
            pltpu.VMEM((D, FF + D), bf16),
            pltpu.VMEM((FF, D), bf16),
            pltpu.SemaphoreType.DMA((3,)),
        ],
        compiler_params=params(),
        cost_estimate=pl.CostEstimate(
            flops=2 * count * ROWS * (2 * D * D + 2 * D * FF), bytes_accessed=70_000_000, transcendentals=0
        ),
        name="back_mlp",
    )(divisor, e, a, f, targets, mask, gp, vectors, wide, second)


def back_attention_kernel(
    dx1, a, e, qkv, lse, msk, vec, wide_hbm, da, dqkv, dbase, acc, d_att, wide, sems
):
    first = pl.program_id(0) == 0
    copies = [
        pltpu.make_async_copy(wide_hbm.at[:, pl.ds(4 * D, D)], wide.at[:, pl.ds(3 * D, D)], sems.at[0]),
        pltpu.make_async_copy(wide_hbm.at[:, pl.ds(D, 3 * D)], wide.at[:, pl.ds(0, 3 * D)], sems.at[1]),
    ]

    def await_copy(i):
        @pl.when(first)
        def _():
            copies[i].wait()

    @pl.when(first)
    def _():
        for item in copies:
            item.start()
        acc[...] = jnp.zeros_like(acc)

    def row(i):
        return vec[i : i + 1, :]

    def add(i, val):
        acc[i : i + 1, :] += val

    count = PAIR * ROWS
    grad = dx1[...].reshape(count, D)
    add(8, col_sum(a[...].reshape(count, D) * grad))
    dbranch = (row(8) * grad).astype(bf16)
    da[...] = dbranch.reshape(PAIR, ROWS, D)
    add(7, col_sum(dbranch.astype(f32)))
    await_copy(0)
    d_att[...] = dot_nt(dbranch, wide[:, 3 * D :]).astype(bf16).reshape(PAIR, ROWS, D)

    lane = lax.broadcasted_iota(jnp.int32, (ROWS, 128), 1)
    low_half = lane < 64
    key_live = lax.broadcasted_iota(jnp.int32, (1, ROWS), 1) <= NP

    def attend(j, carry):
        for p in range(HEADS // 2):
            cols = slice(128 * p, 128 * (p + 1))
            q2 = qkv[j, :, 128 * p : 128 * (p + 1)]
            k2 = qkv[j, :, D + 128 * p : D + 128 * (p + 1)]
            v2 = qkv[j, :, 2 * D + 128 * p : 2 * D + 128 * (p + 1)]
            do2 = d_att[j, :, cols]
            dq, dk, dv = [], [], []
            for half in range(2):
                pick = low_half if half == 0 else ~low_half
                zero = jnp.zeros_like(q2)
                s = dot_nt(jnp.where(pick, q2, zero), k2) * HEAD_SCALE
                soft = jnp.where(key_live, jnp.exp(s - lse[j, :, 2 * p + half : 2 * p + half + 1]), 0.0)
                dsoft = dot_nt(jnp.where(pick, do2, zero), v2)
                dv.append(dot_tn(soft.astype(bf16), do2))
                dscore = soft * (dsoft - jnp.sum(dsoft * soft, axis=-1, keepdims=True))
                dscore = dscore.astype(bf16)
                dq.append(dot_nn(dscore, k2))
                dk.append(dot_tn(dscore, q2))
            dqkv[j, :, 128 * p : 128 * (p + 1)] = (jnp.where(low_half, dq[0], dq[1]) * HEAD_SCALE).astype(bf16)
            dqkv[j, :, D + 128 * p : D + 128 * (p + 1)] = (
                jnp.where(low_half, dk[0], dk[1]) * HEAD_SCALE
            ).astype(bf16)
            dqkv[j, :, 2 * D + 128 * p : 2 * D + 128 * (p + 1)] = jnp.where(low_half, dv[0], dv[1]).astype(bf16)
        return carry

    lax.fori_loop(0, PAIR, attend, 0)
    add(5, col_sum(dqkv[:, :, :D].reshape(count, D).astype(f32)))
    add(6, col_sum(dqkv[:, :, 2 * D :].reshape(count, D).astype(f32)))
    await_copy(1)
    dh = dot_nt(dqkv[...].reshape(count, 3 * D), wide[:, : 3 * D])
    unit, inverse = normed(e[...].reshape(count, D))
    add(3, col_sum(dh * unit))
    add(4, col_sum(dh))
    d_start = dx1[...].reshape(count, D) + norm_back(dh * row(3), unit, inverse)
    place = lax.broadcasted_iota(jnp.int32, (PAIR, ROWS, 1), 1).reshape(count, 1)
    hit = msk[...].reshape(count, 1) > 0.5
    add(0, col_sum(jnp.where(place == NP, d_start, 0.0)))
    add(1, col_sum(jnp.where(hit, d_start, 0.0)))
    kept = jnp.where(hit | (place >= NP), 0.0, d_start).astype(bf16)
    add(2, col_sum(kept.astype(f32)))
    dbase[...] = kept.reshape(PAIR, ROWS, D)


def back_attention(dx1, a, e, qkv, lse, mask, vectors, wide):
    count = e.shape[0]
    return pl.pallas_call(
        back_attention_kernel,
        grid=(count // PAIR,),
        in_specs=[
            pairs(ROWS, D), pairs(ROWS, D), pairs(ROWS, D), pairs(ROWS, 3 * D), pairs(ROWS, 128), pairs(ROWS, 1),
            whole((20, D)), ANY,
        ],
        out_specs=[pairs(ROWS, D), pairs(ROWS, 3 * D), pairs(ROWS, D), whole((16, D))],
        out_shape=[
            jax.ShapeDtypeStruct((count, ROWS, D), bf16),
            jax.ShapeDtypeStruct((count, ROWS, 3 * D), bf16),
            jax.ShapeDtypeStruct((count, ROWS, D), bf16),
            jax.ShapeDtypeStruct((16, D), f32),
        ],
        scratch_shapes=[
            pltpu.VMEM((PAIR, ROWS, D), bf16),
            pltpu.VMEM((D, 4 * D), bf16),
            pltpu.SemaphoreType.DMA((2,)),
        ],
        compiler_params=params(),
        cost_estimate=pl.CostEstimate(
            flops=2 * count * ROWS * (4 * D * D + 10 * ROWS * D), bytes_accessed=40_000_000, transcendentals=0
        ),
        name="back_attention",
    )(dx1, a, e, qkv, lse, mask, vectors, wide)


def weight_grad(rows_in, grads):
    return jnp.einsum("bsd,bse->de", rows_in, grads, preferred_element_type=f32)
CHUNK = 256
SLOTS = 8
AHEAD = 2
LAG = 2
MESH = pl.DeviceIdType.MESH


def bit_orders(m):
    left = list(range(m - 1, -1, -1))
    return left, left[m // 2 :] + left[: m // 2]


LHS_ROWS = 8 * ROWS
RING = 4


def reduce_kernel(m, rows, groups, *refs):
    n_lhs = len(groups)
    lhs_in, rhs_in, refs = refs[:n_lhs], refs[n_lhs : 2 * n_lhs], refs[2 * n_lhs :]
    (extra_in, fc_in, wide_out, fc_out, norm_out), scratch = refs[:5], refs[5:]
    work, core_in, acc, grad, lhs, rhs, held, extra = scratch[:8]
    stage_in = scratch[8 : 8 + m]
    za, zb, nbuf = scratch[8 + m : 11 + m]
    (lhs_s, rhs_s, held_s, extra_s, core_s, core_r, half_s, half_r, chain_s, chain_r, out_s, n_s, n_r) = scratch[11 + m :]
    starts = [sum(g[0] for g in groups[:i]) for i in range(n_lhs + 1)]
    last = starts[-1]
    count = last + 1
    fc_cols = D // CHUNK
    n_held = 4 * fc_cols
    half = CHUNK // 2
    dp, z = lax.axis_index("dp"), lax.axis_index("view")
    core = dp % 2
    own = [(dp // (2 ** (m - d))) % 2 for d in range(m)]
    partner = (dp + 1 - 2 * core, z)
    peers = [(dp + (1 - 2 * own[d]) * 2 ** (m - d), z) for d in range(m)]
    outer = (z == 0) | (z == 3)
    inner = (z == 1) | (z == 2)
    to_inner = (dp, 1 + z // 3)
    to_outer = (dp, (z - 1) * 3)
    across = (dp, 3 - z)
    orders = bit_orders(m)
    full = (slice(None),) * m

    def remote(src, dst, send, recv, device):
        return pltpu.make_async_remote_copy(
            src_ref=src, dst_ref=dst, send_sem=send, recv_sem=recv, device_id=device, device_id_type=MESH
        )

    def local(src, dst, sem):
        return pltpu.make_async_copy(src, dst, sem)

    def slot(k):
        return lax.rem(k, SLOTS)

    def ring(k):
        return lax.rem(k, RING)

    def guarded(k, limit, step):
        @pl.when((k >= 0) & (k < limit))
        def _():
            step(k)

    def at_chunk(k):
        return pl.ds(pl.multiple_of(k * CHUNK, CHUNK), CHUNK)

    def lhs_load(g):
        dst = lhs.at[g % 2]
        repeats = groups[g][2]
        if repeats == 1:
            return [local(lhs_in[g], dst, lhs_s.at[g % 2])]
        return [
            local(lhs_in[g].at[i // repeats], dst.at[pl.ds(i * ROWS, ROWS)], lhs_s.at[g % 2])
            for i in range(LHS_ROWS // ROWS)
        ]

    def rhs_load(k):
        for g in range(n_lhs):

            @pl.when((k >= starts[g]) & (k < starts[g + 1]))
            def _():
                local(rhs_in[g].at[:, at_chunk(k - starts[g])], rhs.at[ring(k)], rhs_s.at[ring(k)]).start()

    local(extra_in, extra, extra_s).start()
    for g in range(2):
        for item in lhs_load(g):
            item.start()
    for k in range(RING - 1):
        rhs_load(jnp.int32(k))

    def held_load(j):
        src = fc_in.at[pl.ds(pl.multiple_of((j // fc_cols) * rows, 8), rows), at_chunk(j % fc_cols)]
        local(src, held.at[j], held_s.at[j]).start()

    def held_all(j, carry):
        held_load(j)
        return carry

    lax.fori_loop(0, n_held, held_all, 0)

    barrier = pltpu.get_barrier_semaphore()
    for peer in [partner] + peers:
        pl.semaphore_signal(barrier, inc=1, device_id=peer, device_id_type=MESH)

    @pl.when(outer)
    def _():
        pl.semaphore_signal(barrier, inc=1, device_id=to_inner, device_id_type=MESH)
        pl.semaphore_wait(barrier, m + 2)

    @pl.when(inner)
    def _():
        pl.semaphore_signal(barrier, inc=1, device_id=to_outer, device_id_type=MESH)
        pl.semaphore_signal(barrier, inc=1, device_id=across, device_id_type=MESH)
        pl.semaphore_wait(barrier, m + 3)

    def hand(k):
        src = grad.at[(ring(k),) + full + (1 - core,)]
        return remote(src, core_in.at[k], core_s.at[slot(k)], core_r.at[slot(k)], partner)

    def compute(k):
        r = ring(k)

        @pl.when(k < last)
        def _():
            group = 0
            for g in range(1, n_lhs):
                group = group + (k >= starts[g]).astype(jnp.int32)
            for g in range(n_lhs):

                @pl.when(k == starts[g])
                def _():
                    local(lhs.at[g % 2], lhs.at[g % 2], lhs_s.at[g % 2]).wait()
                    if 1 <= g < n_lhs - 1:
                        for item in lhs_load(g + 1):
                            item.start()

            local(rhs.at[r], rhs.at[r], rhs_s.at[r]).wait()
            val = dot_tn(lhs[group % 2], rhs[r])
            grad[r] = val.reshape((2,) * (m + 1) + (rows, CHUNK))

        @pl.when(k == last)
        def _():
            local(extra_in, extra, extra_s).wait()
            grad[r] = extra[...]

        @pl.when(k + RING - 1 < last)
        def _():
            rhs_load(k + RING - 1)

        hand(k).start()

    def lead(order, stage, flip):
        out = []
        for d in range(m):
            if d in order[:stage]:
                out.append(own[d])
            elif d == order[stage]:
                out.append(1 - own[d] if flip else own[d])
            else:
                out.append(slice(None))
        return tuple(out)

    def exchange(k, stage, side):
        order = orders[side]
        s = slot(k)
        cols = slice(side * half, (side + 1) * half)
        return remote(
            work.at[(k,) + lead(order, stage, True) + (slice(None), cols)],
            stage_in[stage].at[k, side],
            half_s.at[s, stage, side],
            half_r.at[s, stage, side],
            peers[order[stage]],
        )

    def by_rows(body):
        def go(i, carry):
            body(pl.ds(pl.multiple_of(i * 8, 8), 8))
            return carry

        lax.fori_loop(0, rows // 8, go, 0)

    def merge_core(k):
        hand(k).wait()

        def body(r):
            at = full + (r, slice(None))
            work[(k,) + at] = grad[(ring(k),) + full + (core, r, slice(None))] + core_in[(k,) + at]

        by_rows(body)
        for side in range(2):
            exchange(k, 0, side).start()

    def merge_stage(k, stage):
        for side in range(2):
            exchange(k, stage, side).wait()
            order = orders[side]
            cols = slice(side * half, (side + 1) * half)

            def body(r):
                at = (k,) + lead(order, stage, False) + (r, cols)
                work[at] = work[at] + stage_in[stage][(k, side) + (slice(None),) * (m - stage - 1) + (r, slice(None))]

            by_rows(body)
            if stage + 1 < m:
                exchange(k, stage + 1, side).start()
        if stage + 1 == m:

            @pl.when(outer)
            def _():
                chain(0, k, 0).start()

    def mine(track, k):
        return work.at[(k,) + tuple(own)] if track == 0 else held.at[k]

    def index(track, k):
        return k if track == 0 else count + k

    def chain(track, k, hop):
        i, s = index(track, k), slot(k)
        src = mine(track, k) if hop < 2 else za.at[i]
        dst = zb.at[i] if hop == 1 else za.at[i]
        device = (to_inner, across, to_outer)[hop]
        return remote(src, dst, chain_s.at[s, track, hop], chain_r.at[s, track, hop], device)

    def open_held(k):
        local(held.at[k], held.at[k], held_s.at[k]).wait()

        @pl.when(outer)
        def _():
            chain(1, k, 0).start()

    def meet(k, track):
        @pl.when(inner)
        def _():
            chain(track, k, 0).wait_recv()
            ref, i = mine(track, k), index(track, k)

            def body(r):
                ref[r, :] = ref[r, :] + za[i, r, :]

            by_rows(body)
            chain(track, k, 1).start()

    def total(k, track):
        @pl.when(inner)
        def _():
            chain(track, k, 1).wait()
            ref, i = mine(track, k), index(track, k)

            def body(r):
                za[i, r, :] = ref[r, :] + zb[i, r, :]

            by_rows(body)
            chain(track, k, 2).start()

    lanes = lax.broadcasted_iota(jnp.int32, (8, CHUNK), 1)

    def finish(k, track):
        i, s = index(track, k), slot(k)

        @pl.when(outer)
        def _():
            chain(track, k, 0).wait_send()
            chain(track, k, 2).wait_recv()

        @pl.when(inner)
        def _():
            chain(track, k, 2).wait_send()

        @pl.when(k >= SLOTS)
        def _():
            local(za.at[i], za.at[i], out_s.at[s, track]).wait()

        if track == 0:
            column = groups[-1][1] + groups[-1][0] + k - last
            for g in range(n_lhs):
                column = jnp.where((k >= starts[g]) & (k < starts[g + 1]), groups[g][1] + k - starts[g], column)
            column = jnp.where(k == last, wide_out.shape[1] // CHUNK - 1, column)
            local(za.at[i], wide_out.at[:, at_chunk(column)], out_s.at[s, track]).start()
            live = (lanes < 20) | (k != last)
        else:

            dst = fc_out.at[pl.ds(pl.multiple_of((k // fc_cols) * rows, 8), rows), at_chunk(k % fc_cols)]
            local(za.at[i], dst, out_s.at[s, track]).start()
            live = None

        def body(r):
            val = za[i, r, :]
            if live is not None:
                val = jnp.where(live, val, 0.0)
            acc[...] += val * val

        by_rows(body)

    acc[...] = jnp.zeros_like(acc)
    for k in range(AHEAD):
        compute(jnp.int32(k))

    def step(t, carry):
        guarded(t, count, merge_core)
        guarded(t, n_held, open_held)
        guarded(t + AHEAD, count, compute)
        for stage in range(m):
            guarded(t - LAG * (stage + 1), count, functools.partial(merge_stage, stage=stage))
        guarded(t - LAG, n_held, functools.partial(meet, track=1))
        guarded(t - LAG * (m + 1), count, functools.partial(meet, track=0))
        guarded(t - 2 * LAG, n_held, functools.partial(total, track=1))
        guarded(t - LAG * (m + 2), count, functools.partial(total, track=0))
        guarded(t - 3 * LAG, n_held, functools.partial(finish, track=1))
        guarded(t - LAG * (m + 3), count, functools.partial(finish, track=0))
        return carry

    lax.fori_loop(0, count + LAG * (m + 3), step, 0)
    for track, size in enumerate((count, n_held)):
        for k in range(size - SLOTS, size):
            local(za.at[0], za.at[0], out_s.at[k % SLOTS, track]).wait()

    nbuf[0] = acc[:, :128] + acc[:, 128:]
    for j, peer in enumerate([partner] + peers):
        copy = remote(nbuf.at[2 * j], nbuf.at[2 * j + 1], n_s.at[j], n_r.at[j], peer)
        copy.start()
        copy.wait()
        nbuf[2 * j + 2] = nbuf[2 * j] + nbuf[2 * j + 1]
    norm_out[...] = nbuf[2 * m + 2]


def reduce_all(products, extra, fc_shard, dp):
    m = dp.bit_length() - 2
    rows = D // dp
    groups, lefts, rights = [], [], []
    for left, right, column in products:
        repeats = right.shape[0] // left.shape[0]
        lefts.append(left if repeats > 1 else left.reshape(LHS_ROWS, D))
        rights.append(right.reshape(LHS_ROWS, right.shape[-1]))
        groups.append((right.shape[-1] // CHUNK, column // CHUNK, repeats))
    count = sum(g[0] for g in groups) + 1
    n_held = 4 * D // CHUNK
    width = 6 * D + FF + CHUNK
    lead = (2,) * m
    dma = pltpu.SemaphoreType.DMA
    vmem = pltpu.VMEM
    return pl.pallas_call(
        functools.partial(reduce_kernel, m, rows, groups),
        in_specs=[ANY] * (2 * len(groups) + 2),
        out_specs=[ANY, ANY, pl.BlockSpec(memory_space=pltpu.VMEM)],
        out_shape=[
            jax.ShapeDtypeStruct((rows, width), f32),
            jax.ShapeDtypeStruct((4 * rows, D), f32),
            jax.ShapeDtypeStruct((8, 128), f32),
        ],
        scratch_shapes=[
            vmem((count,) + lead + (rows, CHUNK), f32),
            vmem((count,) + lead + (rows, CHUNK), f32),
            vmem((8, CHUNK), f32),
            vmem((RING,) + lead + (2, rows, CHUNK), f32),
            vmem((2, LHS_ROWS, D), bf16),
            vmem((RING, LHS_ROWS, CHUNK), bf16),
            vmem((n_held, rows, CHUNK), f32),
            vmem(lead + (2, rows, CHUNK), f32),
        ]
        + [vmem((count, 2) + (2,) * (m - s - 1) + (rows, CHUNK // 2), f32) for s in range(m)]
        + [
            vmem((count + n_held, rows, CHUNK), f32),
            vmem((count + n_held, rows, CHUNK), f32),
            vmem((2 * m + 3, 8, 128), f32),
            dma((2,)), dma((RING,)), dma((n_held,)), dma, dma((SLOTS,)), dma((SLOTS,)),
            dma((SLOTS, m, 2)), dma((SLOTS, m, 2)), dma((SLOTS, 2, 3)), dma((SLOTS, 2, 3)), dma((SLOTS, 2)),
            dma((m + 1,)), dma((m + 1,)),
        ],
        compiler_params=pltpu.CompilerParams(
            vmem_limit_bytes=VMEM_BYTES, collective_id=0, has_side_effects=True
        ),
        cost_estimate=pl.CostEstimate(
            flops=2 * LHS_ROWS * D * CHUNK * count, bytes_accessed=60_000_000, transcendentals=0
        ),
        name="reduce_gradients",
    )(
        *lefts, *rights, extra.reshape(lead + (2, rows, CHUNK)), fc_shard
    )


def gather_kernel(m, flows, freqs, *refs):
    n_arr = 1 + max(a for a, _, _, _ in flows)
    ins, outs, table = refs[:n_arr], refs[n_arr : 2 * n_arr], refs[2 * n_arr]
    own_s, step_s, step_r, core_s, core_r = refs[2 * n_arr + 1 :]
    dp, z = lax.axis_index("dp"), lax.axis_index("view")
    core = dp % 2
    own = [(dp // (2 ** (m - d))) % 2 for d in range(m)]
    partner = (dp + 1 - 2 * core, z)
    peers = [(dp + (1 - 2 * own[d]) * 2 ** (m - d), z) for d in range(m)]
    orders = bit_orders(m)

    barrier = pltpu.get_barrier_semaphore()
    for peer in [partner] + peers:
        pl.semaphore_signal(barrier, inc=1, device_id=peer, device_id_type=MESH)
    pl.semaphore_wait(barrier, m + 1)

    def remote(src, dst, send, recv, device):
        return pltpu.make_async_remote_copy(
            src_ref=src, dst_ref=dst, send_sem=send, recv_sem=recv, device_id=device, device_id_type=MESH
        )

    def region(i, known, flip=None, which=core):
        a, lo, hi, _ = flows[i]
        lead = tuple(slice(None) if d in known else (1 - own[d] if d == flip else own[d]) for d in range(m))
        return outs[a].at[lead + (which, slice(None), pl.ds(lo, hi - lo))]

    def mine(i):
        a, lo, hi, _ = flows[i]
        return ins[a].at[:, pl.ds(lo, hi - lo)]

    def send(i, s):
        order = orders[flows[i][3]]
        src = mine(i) if s == 0 else region(i, order[:s])
        return remote(src, region(i, order[:s]), step_s.at[i, s], step_r.at[i, s], peers[order[s]])

    def arrive(i, s):
        order = orders[flows[i][3]]
        ref = region(i, order[:s], order[s])
        return remote(ref, ref, step_s.at[i, s], step_r.at[i, s], peers[order[s]])

    def hand_over(i, s):
        order = orders[flows[i][3]]
        if s == 0:
            return remote(mine(i), region(i, ()), core_s.at[i, 0], core_r.at[i, 0], partner)
        ref = region(i, order[: s - 1], order[s - 1])
        return remote(ref, ref, core_s.at[i, s], core_r.at[i, s], partner)

    def taken(i, s):
        order = orders[flows[i][3]]
        ref = region(i, (), None, 1 - core) if s == 0 else region(i, order[: s - 1], order[s - 1], 1 - core)
        return remote(ref, ref, core_s.at[i, s], core_r.at[i, s], partner)

    count = len(flows)
    for i in range(count):
        send(i, 0).start()
    keeps = [
        pltpu.make_async_copy(ins[a], outs[a].at[tuple(own) + (core,)], own_s.at[a]) for a in range(n_arr)
    ]
    for keep in keeps:
        keep.start()
    for i in range(count):
        hand_over(i, 0).start()

    odd = lax.broadcasted_iota(jnp.int32, (8, D), 1) % 2 == 1

    def fill(i, carry):
        at = i * 8 + lax.broadcasted_iota(jnp.int32, (8, D), 0)
        place = jnp.where(at < NP, at + 1, 0)
        angle = place.astype(f32) * freqs[...]
        val = jnp.where(odd, jnp.cos(angle), jnp.sin(angle))
        table[pl.ds(pl.multiple_of(i * 8, 8), 8), :] = jnp.where(at <= NP, val, 0.0)
        return carry

    lax.fori_loop(0, ROWS // 8, fill, 0)
    for keep in keeps:
        keep.wait()
    for s in range(m):
        for i in range(count):
            arrive(i, s).wait_recv()
            if s + 1 < m:
                send(i, s + 1).start()
            hand_over(i, s + 1).start()
    for i in range(count):
        for s in range(m):
            send(i, s).wait_send()
        for s in range(m + 1):
            hand_over(i, s).wait_send()
            taken(i, s).wait_recv()


def gather_weights(freqs, arrays, dp):
    m = dp.bit_length() - 2
    flows = []
    for a, item in enumerate(arrays):
        cols = item.shape[1]
        if cols >= 2 * 128:
            flows += [(a, 0, cols // 2, 0), (a, cols // 2, cols, 1)]
        else:
            flows.append((a, 0, cols, 0))
    lead = (2,) * m + (2,)
    dma = pltpu.SemaphoreType.DMA
    vmem = pl.BlockSpec(memory_space=pltpu.VMEM)
    count = len(flows)
    *full, table = pl.pallas_call(
        functools.partial(gather_kernel, m, flows),
        in_specs=[vmem] * (1 + len(arrays)),
        out_specs=[ANY] * len(arrays) + [vmem],
        out_shape=[jax.ShapeDtypeStruct(lead + item.shape, item.dtype) for item in arrays]
        + [jax.ShapeDtypeStruct((ROWS, D), f32)],
        scratch_shapes=[
            dma((len(arrays),)),
            dma((count, m)),
            dma((count, m)),
            dma((count, m + 1)),
            dma((count, m + 1)),
        ],
        compiler_params=pltpu.CompilerParams(
            vmem_limit_bytes=VMEM_BYTES, collective_id=1, has_side_effects=True
        ),
        cost_estimate=pl.CostEstimate(flops=1_000_000, bytes_accessed=20_000_000, transcendentals=400_000),
        name="gather_weights",
    )(freqs, *arrays)
    return [item.reshape((dp * item.shape[-2], item.shape[-1])) for item in full], table


def adam_step(grad_in, first, second, master, rate, decay, bias_one, bias_two):
    first_new = beta_one * first + (1.0 - beta_one) * grad_in
    second_new = beta_two * second + (1.0 - beta_two) * grad_in * grad_in
    ratio = first_new / bias_one / (jnp.sqrt(second_new / bias_two) + adam_eps)
    return (master - rate * (ratio + decay * master), first_new, second_new)


def update_all(grad_list, first_list, second_list, master_list, factor, bias_one, bias_two):
    rates = (rate_matrix, rate_matrix, rate_vector)
    decays = (decay_matrix, decay_matrix, 0.0)
    results = []
    for index in range(3):
        results.extend(
            adam_step(
                grad_list[index] * factor,
                first_list[index],
                second_list[index],
                master_list[index],
                rates[index],
                decays[index],
                bias_one,
                bias_two,
            )
        )
    return results


def body(
    pixels,
    patch_masks,
    teacher_wide,
    teacher_fc2,
    teacher_vec,
    student_wide,
    student_fc2,
    student_vec,
    wide_first,
    wide_second,
    fc2_first,
    fc2_second,
    vec_first,
    vec_second,
    step_count,
):
    view_id = lax.axis_index("view")
    view_count = lax.axis_size("view")
    group_size = pixels.shape[0]
    owned_images = group_size // view_count
    t_wide, t_second = (
        lax.all_gather(teacher_wide, "dp", axis=0, tiled=True),
        lax.all_gather(teacher_fc2, "dp", axis=0, tiled=True),
    )
    masked = jnp.sum(patch_masks).astype(f32)
    small = jnp.concatenate(
        [
            student_vec.astype(bf16).astype(f32),
            teacher_vec.astype(f32),
            jnp.broadcast_to(masked, (1, student_vec.shape[1])),
            jnp.zeros((128 - 41, student_vec.shape[1]), f32),
        ],
        axis=0,
    ).T
    shards = lax.axis_size("dp")
    (s_wide, s_second, tables), table = gather_weights(
        frequencies(), (student_wide.astype(bf16), student_fc2.astype(bf16), small), shards
    )
    tables = tables.T
    s_vectors, t_vectors = tables[:20], tables[20:40]
    masked_total = jnp.sum(tables[40, :: D // shards])
    divisor = masked_total * math.sqrt(D)
    own_pixels = lax.dynamic_slice_in_dim(pixels, view_id * owned_images, owned_images, 0)
    own_masks = lax.dynamic_slice_in_dim(patch_masks, view_id * owned_images, owned_images, 0)
    own_masks = own_masks.reshape(owned_images * view_count, NP)
    mask = jnp.pad(own_masks.astype(f32), ((0, 0), (0, ROWS - NP)))[:, :, None]
    e, h, qkv, lse, o, a, h2, gp, g, f = forward(
        False, own_pixels, mask, table, s_vectors, s_wide, s_second
    )
    targets = forward(True, own_pixels, None, table, t_vectors, t_wide, t_second)
    y, dpred, df, du, dx1, acc_mlp, acc_b1 = back_mlp(
        divisor.reshape(1, 1), e, a, f, targets, mask, gp, s_vectors, s_wide, s_second
    )
    fc_shard = lax.psum_scatter(weight_grad(g, df), "dp", scatter_dimension=0, tiled=True)
    da, dqkv, dbase, acc_att = back_attention(dx1, a, e, qkv, lse, mask, s_vectors, s_wide)
    loss_part = jnp.sum(acc_mlp[0])
    g_vec = jnp.concatenate([acc_att[:9], acc_mlp[9:], acc_b1.reshape(-1, D)], axis=0)
    extra = jnp.concatenate([g_vec, jnp.broadcast_to(loss_part, (1, D)), jnp.zeros((CHUNK - 21, D), f32)], axis=0)
    steps_done = step_count[0].astype(f32)
    bias_one = 1.0 - jnp.power(beta_one, steps_done)
    bias_two = 1.0 - jnp.power(beta_two, steps_done)
    wide_all, shard_second, squares = reduce_all(
        (
            (h2, du, 5 * D),
            (y, dpred, 5 * D + FF),
            (o, da, 4 * D),
            (h, dqkv, D),
            (jnp.pad(own_pixels, ((0, 0), (0, ROWS - NP), (0, 0))), dbase, 0),
        ),
        extra.T,
        fc_shard,
        shards,
    )
    width = student_wide.shape[1]
    shard_wide, shard_vec = wide_all[:, :width], wide_all[:, width : width + 20].T
    loss_all = wide_all[0, width + 20]
    grad_list = (shard_wide, shard_second, shard_vec)
    grad_norm = jnp.sqrt(jnp.sum(squares))
    factor = jnp.minimum(1.0, clip_limit / grad_norm)
    results = update_all(
        grad_list,
        (wide_first, fc2_first, vec_first),
        (wide_second, fc2_second, vec_second),
        (student_wide, student_fc2, student_vec),
        factor,
        bias_one,
        bias_two,
    )
    return ((loss_all / divisor).reshape(1), grad_norm.reshape(1), *results)


def solution(mesh):
    in_specs = (
        P("dp", None, None),
        P("dp", None, None),
        P("dp", None),
        P("dp", None),
        P(None, "dp"),
        P("dp", None),
        P("dp", None),
        P(None, "dp"),
        P("dp", None),
        P("dp", None),
        P("dp", None),
        P("dp", None),
        P(None, "dp"),
        P(None, "dp"),
        P(),
    )
    out_specs = (
        P(),
        P(),
        P("dp", None),
        P("dp", None),
        P("dp", None),
        P("dp", None),
        P("dp", None),
        P("dp", None),
        P(None, "dp"),
        P(None, "dp"),
        P(None, "dp"),
    )
    return jax.shard_map(body, mesh=mesh, in_specs=in_specs, out_specs=out_specs, check_vma=False)
```

```python
import functools
import math

import jax
import jax.numpy as jnp
from jax import lax
from jax.experimental import pallas as pl
from jax.experimental.pallas import tpu as pltpu
from jax.sharding import PartitionSpec as P

D = 768
HEADS = 12
FF = 3072
NP = 196
ROWS = 208
PAIR = 2
HEAD_SCALE = (D // HEADS) ** (-0.5)

norm_eps = 1e-06
target_eps = 1e-05
smooth_beta = 2.0
clip_limit = 0.004
beta_one = 0.9
beta_two = 0.999
adam_eps = 1e-08
rate_matrix = 0.03
rate_vector = 0.2
decay_matrix = 0.05

f32 = jnp.float32
bf16 = jnp.bfloat16
VMEM_BYTES = 66 * 1024 * 1024 - 2 * 1024 * 1024 - 65536


def dot_nn(a, b):
    return jnp.dot(a, b, preferred_element_type=f32)


def dot_nt(a, b):
    return lax.dot_general(a, b, (((1,), (1,)), ((), ())), preferred_element_type=f32)


def dot_tn(a, b):
    return lax.dot_general(a, b, (((0,), (0,)), ((), ())), preferred_element_type=f32)


def frequencies():
    index = (jnp.arange(D) // 2).astype(f32)
    return jnp.exp(index * (-2.0 * math.log(10000.0) / D)).reshape(1, D)


def normed(values):
    center = values - jnp.mean(values, axis=-1, keepdims=True)
    inverse = lax.rsqrt(jnp.mean(center * center, axis=-1, keepdims=True) + norm_eps)
    return center * inverse, inverse


def norm_back(scaled, unit, inverse):
    return inverse * (
        scaled
        - jnp.mean(scaled, axis=-1, keepdims=True)
        - unit * jnp.mean(scaled * unit, axis=-1, keepdims=True)
    )


def col_sum(values):
    return jnp.sum(values, axis=0, keepdims=True)


def forward_kernel(teacher, travel, *refs):
    if teacher:
        (pix, tab, vec, b1, wide_hbm, w2_hbm, tgt, e, qkv, o, g, wide, w2, sems) = refs
    else:
        (pix, msk, tab, vec, b1, wide_hbm, w2_hbm, next_wide, next_w2) = refs[:9]
        (e, h, qkv, lse, o, a, h2, gp, g, f, full_wide, full_w2, wide, w2, sems) = refs[9:24]
        flows, early, late, m = travel
        begin, kept, advance, close = gather_steps(
            m, flows, (next_wide, next_w2), (full_wide, full_w2), refs[24:]
        )

    def at_step(i, *acts):
        if not teacher:

            @pl.when(pl.program_id(0) == i)
            def _():
                for act in acts:
                    act()

    cuts = (0, D, 4 * D, 5 * D, 5 * D + FF)
    first = pl.program_id(0) == 0
    copies = [
        pltpu.make_async_copy(
            wide_hbm.at[:, pl.ds(cuts[i], cuts[i + 1] - cuts[i])],
            wide.at[:, pl.ds(cuts[i], cuts[i + 1] - cuts[i])],
            sems.at[i],
        )
        for i in range(4)
    ] + [pltpu.make_async_copy(w2_hbm, w2, sems.at[4])]

    def await_copy(i):
        @pl.when(first)
        def _():
            copies[i].wait()

    @pl.when(first)
    def _():
        for item in copies:
            item.start()

    def row(i):
        return vec[i : i + 1, :]

    if not teacher:
        final_step = pl.num_programs(0) - 1
        at_step(0, lambda: greet_gather(m), begin)
        at_step(1, kept, lambda: advance(early, 0))
        at_step(final_step, *[functools.partial(advance, early, s) for s in range(1, m)])
    await_copy(0)
    for j in range(PAIR):
        if teacher or j == 0:
            patches = dot_nn(pix[j], wide[:, :D]) + row(2)
        base = patches if teacher else jnp.where(msk[j, :NP, :] > 0.5, row(1), patches)
        sub = lax.broadcasted_iota(jnp.int32, (16, D), 0)
        e[j, ROWS - 16 :, :] = jnp.where(sub == NP - (ROWS - 16), row(0) + tab[NP : NP + 1, :], 0.0)
        e[j, :NP, :] = base + tab[:NP, :]
    start = e[...].reshape(PAIR * ROWS, D)
    unit, _ = normed(start)
    hidden = (unit * row(3) + row(4)).astype(bf16)
    if not teacher:
        h[...] = hidden.reshape(PAIR, ROWS, D)
    await_copy(1)
    for part, bias in enumerate((5, None, 6)):
        val = dot_nn(hidden, wide[:, D * (part + 1) : D * (part + 2)])
        if bias is not None:
            val = val + row(bias)
        qkv[:, :, D * part : D * (part + 1)] = val.astype(bf16).reshape(PAIR, ROWS, D)

    lane = lax.broadcasted_iota(jnp.int32, (ROWS, 128), 1)
    low_half = lane < 64
    key_bias = jnp.where(lax.broadcasted_iota(jnp.int32, (1, ROWS), 1) <= NP, 0.0, -1e30)

    def attend(j, carry):
        logs = jnp.zeros((ROWS, 128), f32)
        for p in range(HEADS // 2):
            q2 = qkv[j, :, 128 * p : 128 * (p + 1)]
            k2 = qkv[j, :, D + 128 * p : D + 128 * (p + 1)]
            v2 = qkv[j, :, 2 * D + 128 * p : 2 * D + 128 * (p + 1)]
            outs = []
            for half in range(2):
                q_one = jnp.where(low_half if half == 0 else ~low_half, q2, jnp.zeros_like(q2))
                s = dot_nt(q_one, k2) * HEAD_SCALE + key_bias
                peak = jnp.max(s, axis=-1, keepdims=True)
                raised = jnp.exp(s - peak)
                total = jnp.sum(raised, axis=-1, keepdims=True)
                outs.append(dot_nn((raised / total).astype(bf16), v2))
                if not teacher:
                    logs = jnp.where(lane == 2 * p + half, peak + jnp.log(total), logs)
            o[j, :, 128 * p : 128 * (p + 1)] = jnp.where(low_half, outs[0], outs[1]).astype(bf16)
        if not teacher:
            lse[j] = logs
        return carry

    lax.fori_loop(0, PAIR, attend, 0)
    if not teacher:
        at_step(1, lambda: advance(late, 0))
    await_copy(2)
    branch = dot_nn(o[...].reshape(PAIR * ROWS, D), wide[:, 4 * D : 5 * D]) + row(7)
    if not teacher:
        a[...] = branch.reshape(PAIR, ROWS, D)
    middle = e[...].reshape(PAIR * ROWS, D) + row(8) * branch
    unit, _ = normed(middle)
    hidden_two = (unit * row(9) + row(10)).astype(bf16)
    if teacher:
        e[...] = middle.reshape(PAIR, ROWS, D)
    else:
        h2[...] = hidden_two.reshape(PAIR, ROWS, D)
    await_copy(3)
    tile = 1024
    for t in range(FF // tile):
        cols = slice(t * tile, (t + 1) * tile)
        pre = dot_nn(hidden_two, wide[:, 5 * D + t * tile : 5 * D + (t + 1) * tile]) + b1[:, cols]
        cumulative = 0.5 * (1.0 + lax.erf(pre * 2.0 ** (-0.5)))
        g[:, :, cols] = (pre * cumulative).astype(bf16).reshape(PAIR, ROWS, tile)
        if not teacher:
            density = jnp.exp(-0.5 * pre * pre) * (2.0 * math.pi) ** (-0.5)
            gp[:, :, cols] = (cumulative + pre * density).reshape(PAIR, ROWS, tile)
    await_copy(4)
    mlp = dot_nn(g[...].reshape(PAIR * ROWS, FF), w2[...]) + row(11)
    if not teacher:
        f[...] = mlp.reshape(PAIR, ROWS, D)
        at_step(final_step, *[functools.partial(advance, late, s) for s in range(1, m)], close)
        return
    final = (e[...].reshape(PAIR * ROWS, D) + row(12) * mlp).reshape(PAIR, ROWS, D)
    e[...] = final
    for j in range(PAIR):
        patch = e[j, :NP, :]
        center = patch - jnp.mean(patch, axis=0, keepdims=True)
        tgt[j, ROWS - 16 :, :] = jnp.zeros((16, D), bf16)
        tgt[j, :NP, :] = (
            center * lax.rsqrt(jnp.mean(center * center, axis=0, keepdims=True) + target_eps)
        ).astype(bf16)


def whole(shape):
    return pl.BlockSpec(shape, lambda i: (0,) * len(shape))


def pairs(rows, cols):
    return pl.BlockSpec((PAIR, rows, cols), lambda i: (i, 0, 0))


ANY = pl.BlockSpec(memory_space=pl.ANY)


def params():
    return pltpu.CompilerParams(vmem_limit_bytes=VMEM_BYTES)


def per_image(rows, cols, pairs_each):
    return pl.BlockSpec((1, rows, cols), lambda i: (i // pairs_each, 0, 0))


def forward(teacher, pixels, mask, table, vectors, wide, second, following=None, dp=None):
    count = pixels.shape[0] if teacher else mask.shape[0]
    pairs_each = max(count // pixels.shape[0] // PAIR, 1)
    b1 = vectors[16:].reshape(1, FF)
    cost = pl.CostEstimate(
        flops=int(2 * count * ROWS * (10 * D * D + 2 * D * FF) * (PAIR * 0 + 1)),
        bytes_accessed=60_000_000 if not teacher else 20_000_000,
        transcendentals=count * ROWS * FF * 2,
    )
    scratch_weights = [
        pltpu.VMEM((D, 5 * D + FF), bf16),
        pltpu.VMEM((FF, D), bf16),
        pltpu.SemaphoreType.DMA((5,)),
    ]
    if teacher:
        return pl.pallas_call(
            functools.partial(forward_kernel, True, None),
            grid=(count // PAIR,),
            in_specs=[pairs(NP, D), whole((ROWS, D)), whole((20, D)), whole((1, FF)), ANY, ANY],
            out_specs=pairs(ROWS, D),
            out_shape=jax.ShapeDtypeStruct((count, ROWS, D), bf16),
            scratch_shapes=[
                pltpu.VMEM((PAIR, ROWS, D), f32),
                pltpu.VMEM((PAIR, ROWS, 3 * D), bf16),
                pltpu.VMEM((PAIR, ROWS, D), bf16),
                pltpu.VMEM((PAIR, ROWS, FF), bf16),
            ]
            + scratch_weights,
            compiler_params=params(),
            cost_estimate=cost,
            name="teacher_forward",
        )(pixels, table, vectors, b1, wide, second)
    kinds = (
        (D, f32),
        (D, bf16),
        (3 * D, bf16),
        (128, f32),
        (D, bf16),
        (D, f32),
        (D, bf16),
        (FF, f32),
        (FF, bf16),
        (D, f32),
    )
    m = dp.bit_length() - 2
    next_wide, next_w2 = following
    width, split = next_wide.shape[1], 7 * 128
    flows = [(1, 0, D // 2, 0), (1, D // 2, D, 1)]
    for side in range(2):
        low = side * width // 2
        flows += [(0, low, low + split, side), (0, low + split, low + width // 2, side)]
    early, late = (0, 1, 2, 4), (3, 5)
    lead = (2,) * (m + 1)
    once = pl.Buffered(1)
    held = [
        pl.BlockSpec(item.shape, lambda i: (0, 0), pipeline_mode=once) for item in following
    ]
    *saved, full_wide, full_w2 = pl.pallas_call(
        functools.partial(forward_kernel, False, (flows, early, late, m)),
        grid=(count // PAIR,),
        in_specs=[
            per_image(NP, D, pairs_each), pairs(ROWS, 1), whole((ROWS, D)), whole((20, D)), whole((1, FF)), ANY, ANY,
            *held,
        ],
        out_specs=[pairs(ROWS, cols) for cols, _ in kinds] + [ANY, ANY],
        out_shape=[jax.ShapeDtypeStruct((count, ROWS, cols), kind) for cols, kind in kinds]
        + [jax.ShapeDtypeStruct(lead + item.shape, item.dtype) for item in following],
        scratch_shapes=scratch_weights + gather_sems(2, len(flows), m),
        compiler_params=pltpu.CompilerParams(
            vmem_limit_bytes=VMEM_BYTES, collective_id=2, has_side_effects=True
        ),
        cost_estimate=cost,
        name="student_forward",
    )(pixels, mask, table, vectors, b1, wide, second, *following)
    return saved, full_wide.reshape(-1, width), full_w2.reshape(-1, D)


def back_mlp_kernel(
    div, e, a, f, tgt, msk, gp, vec, wide_hbm, w2_hbm,
    y, dpred, df, du, dx1, acc, accb, wide, w2, sems,
):
    first = pl.program_id(0) == 0
    copies = [
        pltpu.make_async_copy(wide_hbm.at[:, pl.ds(5 * D + FF, D)], wide.at[:, pl.ds(FF, D)], sems.at[0]),
        pltpu.make_async_copy(w2_hbm, w2, sems.at[1]),
        pltpu.make_async_copy(wide_hbm.at[:, pl.ds(5 * D, FF)], wide.at[:, pl.ds(0, FF)], sems.at[2]),
    ]

    def await_copy(i):
        @pl.when(first)
        def _():
            copies[i].wait()

    @pl.when(first)
    def _():
        for item in copies:
            item.start()
        acc[...] = jnp.zeros_like(acc)
        accb[...] = jnp.zeros_like(accb)

    def row(i):
        return vec[i : i + 1, :]

    def add(i, val):
        acc[i : i + 1, :] += val

    count = PAIR * ROWS
    middle = e[...].reshape(count, D) + row(8) * a[...].reshape(count, D)
    mlp = f[...].reshape(count, D)
    unit, inverse = normed(middle + row(12) * mlp)
    rows_in = (unit * row(13) + row(14)).astype(bf16)
    y[...] = rows_in.reshape(PAIR, ROWS, D)
    await_copy(0)
    goal = jnp.broadcast_to(tgt[...].astype(f32), (PAIR, ROWS, D)).reshape(count, D)
    gap = dot_nn(rows_in, wide[:, FF:]) + row(15) - goal
    live = msk[...].reshape(count, 1) > 0.5
    size = jnp.abs(gap)
    terms = jnp.where(size < smooth_beta, 0.5 * gap * gap / smooth_beta, size - 0.5 * smooth_beta)
    add(0, col_sum(jnp.where(live, terms, 0.0)))
    slope = jnp.where(live, jnp.clip(gap / smooth_beta, -1.0, 1.0) / div[0, 0], 0.0).astype(bf16)
    dpred[...] = slope.reshape(PAIR, ROWS, D)
    add(15, col_sum(slope.astype(f32)))
    dy = dot_nt(slope, wide[:, FF:]).astype(bf16).astype(f32)
    add(13, col_sum(dy * unit))
    add(14, col_sum(dy))
    dx2 = norm_back(dy * row(13), unit, inverse)
    add(12, col_sum(mlp * dx2))
    dmlp = (row(12) * dx2).astype(bf16)
    df[...] = dmlp.reshape(PAIR, ROWS, D)
    add(11, col_sum(dmlp.astype(f32)))
    dx1[...] = dx2.reshape(PAIR, ROWS, D)
    await_copy(1)
    tile = 1024
    for t in range(FF // tile):
        cols = slice(t * tile, (t + 1) * tile)
        val = dot_nt(dmlp, w2[cols, :]) * gp[:, :, cols].reshape(count, tile)
        val = val.astype(bf16)
        du[:, :, cols] = val.reshape(PAIR, ROWS, tile)
        accb[:, cols] += col_sum(val.astype(f32))
    await_copy(2)
    dh2 = dot_nt(du[...].reshape(count, FF), wide[:, :FF])
    middle = e[...].reshape(count, D) + row(8) * a[...].reshape(count, D)
    unit, inverse = normed(middle)
    add(9, col_sum(dh2 * unit))
    add(10, col_sum(dh2))
    grad = dx1[...].reshape(count, D) + norm_back(dh2 * row(9), unit, inverse)
    dx1[...] = grad.reshape(PAIR, ROWS, D)


def back_mlp(divisor, e, a, f, targets, mask, gp, vectors, wide, second):
    count = e.shape[0]
    pairs_each = count // targets.shape[0] // PAIR
    kinds = ((D, bf16), (D, bf16), (D, bf16), (FF, bf16), (D, f32))
    return pl.pallas_call(
        back_mlp_kernel,
        grid=(count // PAIR,),
        in_specs=[
            pl.BlockSpec(memory_space=pltpu.SMEM),
            pairs(ROWS, D), pairs(ROWS, D), pairs(ROWS, D), per_image(ROWS, D, pairs_each), pairs(ROWS, 1),
            pairs(ROWS, FF),
            whole((20, D)), ANY, ANY,
        ],
        out_specs=[pairs(ROWS, cols) for cols, _ in kinds] + [whole((16, D)), whole((1, FF))],
        out_shape=[jax.ShapeDtypeStruct((count, ROWS, cols), kind) for cols, kind in kinds]
        + [jax.ShapeDtypeStruct((16, D), f32), jax.ShapeDtypeStruct((1, FF), f32)],
        scratch_shapes=[
            pltpu.VMEM((D, FF + D), bf16),
            pltpu.VMEM((FF, D), bf16),
            pltpu.SemaphoreType.DMA((3,)),
        ],
        compiler_params=params(),
        cost_estimate=pl.CostEstimate(
            flops=2 * count * ROWS * (2 * D * D + 2 * D * FF), bytes_accessed=70_000_000, transcendentals=0
        ),
        name="back_mlp",
    )(divisor, e, a, f, targets, mask, gp, vectors, wide, second)


def back_attention_kernel(
    dx1, a, e, qkv, lse, msk, vec, wide_hbm, da, dqkv, dbase, acc, d_att, wide, sems
):
    first = pl.program_id(0) == 0
    copies = [
        pltpu.make_async_copy(wide_hbm.at[:, pl.ds(4 * D, D)], wide.at[:, pl.ds(3 * D, D)], sems.at[0]),
        pltpu.make_async_copy(wide_hbm.at[:, pl.ds(D, 3 * D)], wide.at[:, pl.ds(0, 3 * D)], sems.at[1]),
    ]

    def await_copy(i):
        @pl.when(first)
        def _():
            copies[i].wait()

    @pl.when(first)
    def _():
        for item in copies:
            item.start()
        acc[...] = jnp.zeros_like(acc)

    def row(i):
        return vec[i : i + 1, :]

    def add(i, val):
        acc[i : i + 1, :] += val

    count = PAIR * ROWS
    grad = dx1[...].reshape(count, D)
    add(8, col_sum(a[...].reshape(count, D) * grad))
    dbranch = (row(8) * grad).astype(bf16)
    da[...] = dbranch.reshape(PAIR, ROWS, D)
    add(7, col_sum(dbranch.astype(f32)))
    await_copy(0)
    d_att[...] = dot_nt(dbranch, wide[:, 3 * D :]).astype(bf16).reshape(PAIR, ROWS, D)

    lane = lax.broadcasted_iota(jnp.int32, (ROWS, 128), 1)
    low_half = lane < 64
    key_live = lax.broadcasted_iota(jnp.int32, (1, ROWS), 1) <= NP

    def attend(j, carry):
        for p in range(HEADS // 2):
            cols = slice(128 * p, 128 * (p + 1))
            q2 = qkv[j, :, 128 * p : 128 * (p + 1)]
            k2 = qkv[j, :, D + 128 * p : D + 128 * (p + 1)]
            v2 = qkv[j, :, 2 * D + 128 * p : 2 * D + 128 * (p + 1)]
            do2 = d_att[j, :, cols]
            dq, dk, dv = [], [], []
            for half in range(2):
                pick = low_half if half == 0 else ~low_half
                zero = jnp.zeros_like(q2)
                s = dot_nt(jnp.where(pick, q2, zero), k2) * HEAD_SCALE
                soft = jnp.where(key_live, jnp.exp(s - lse[j, :, 2 * p + half : 2 * p + half + 1]), 0.0)
                dsoft = dot_nt(jnp.where(pick, do2, zero), v2)
                dv.append(dot_tn(soft.astype(bf16), do2))
                dscore = soft * (dsoft - jnp.sum(dsoft * soft, axis=-1, keepdims=True))
                dscore = dscore.astype(bf16)
                dq.append(dot_nn(dscore, k2))
                dk.append(dot_tn(dscore, q2))
            dqkv[j, :, 128 * p : 128 * (p + 1)] = (jnp.where(low_half, dq[0], dq[1]) * HEAD_SCALE).astype(bf16)
            dqkv[j, :, D + 128 * p : D + 128 * (p + 1)] = (
                jnp.where(low_half, dk[0], dk[1]) * HEAD_SCALE
            ).astype(bf16)
            dqkv[j, :, 2 * D + 128 * p : 2 * D + 128 * (p + 1)] = jnp.where(low_half, dv[0], dv[1]).astype(bf16)
        return carry

    lax.fori_loop(0, PAIR, attend, 0)
    add(5, col_sum(dqkv[:, :, :D].reshape(count, D).astype(f32)))
    add(6, col_sum(dqkv[:, :, 2 * D :].reshape(count, D).astype(f32)))
    await_copy(1)
    dh = dot_nt(dqkv[...].reshape(count, 3 * D), wide[:, : 3 * D])
    unit, inverse = normed(e[...].reshape(count, D))
    add(3, col_sum(dh * unit))
    add(4, col_sum(dh))
    d_start = dx1[...].reshape(count, D) + norm_back(dh * row(3), unit, inverse)
    place = lax.broadcasted_iota(jnp.int32, (PAIR, ROWS, 1), 1).reshape(count, 1)
    hit = msk[...].reshape(count, 1) > 0.5
    add(0, col_sum(jnp.where(place == NP, d_start, 0.0)))
    add(1, col_sum(jnp.where(hit, d_start, 0.0)))
    kept = jnp.where(hit | (place >= NP), 0.0, d_start).astype(bf16)
    add(2, col_sum(kept.astype(f32)))
    dbase[...] = kept.reshape(PAIR, ROWS, D)


def back_attention(dx1, a, e, qkv, lse, mask, vectors, wide):
    count = e.shape[0]
    return pl.pallas_call(
        back_attention_kernel,
        grid=(count // PAIR,),
        in_specs=[
            pairs(ROWS, D), pairs(ROWS, D), pairs(ROWS, D), pairs(ROWS, 3 * D), pairs(ROWS, 128), pairs(ROWS, 1),
            whole((20, D)), ANY,
        ],
        out_specs=[pairs(ROWS, D), pairs(ROWS, 3 * D), pairs(ROWS, D), whole((16, D))],
        out_shape=[
            jax.ShapeDtypeStruct((count, ROWS, D), bf16),
            jax.ShapeDtypeStruct((count, ROWS, 3 * D), bf16),
            jax.ShapeDtypeStruct((count, ROWS, D), bf16),
            jax.ShapeDtypeStruct((16, D), f32),
        ],
        scratch_shapes=[
            pltpu.VMEM((PAIR, ROWS, D), bf16),
            pltpu.VMEM((D, 4 * D), bf16),
            pltpu.SemaphoreType.DMA((2,)),
        ],
        compiler_params=params(),
        cost_estimate=pl.CostEstimate(
            flops=2 * count * ROWS * (4 * D * D + 10 * ROWS * D), bytes_accessed=40_000_000, transcendentals=0
        ),
        name="back_attention",
    )(dx1, a, e, qkv, lse, mask, vectors, wide)


def weight_grad(rows_in, grads):
    return jnp.einsum("bsd,bse->de", rows_in, grads, preferred_element_type=f32)
CHUNK = 256
SLOTS = 8
AHEAD = 2
LAG = 2
MESH = pl.DeviceIdType.MESH


def bit_orders(m):
    left = list(range(m - 1, -1, -1))
    return left, left[m // 2 :] + left[: m // 2]


LHS_ROWS = 8 * ROWS
RING = 4


def reduce_kernel(m, rows, groups, *refs):
    n_lhs = len(groups)
    lhs_in, rhs_in, refs = refs[:n_lhs], refs[n_lhs : 2 * n_lhs], refs[2 * n_lhs :]
    (extra_in, fc_in, wide_out, fc_out, norm_out), scratch = refs[:5], refs[5:]
    work, core_in, acc, grad, lhs, rhs, held, extra = scratch[:8]
    stage_in = scratch[8 : 8 + m]
    za, zb, nbuf = scratch[8 + m : 11 + m]
    (lhs_s, rhs_s, held_s, extra_s, core_s, core_r, half_s, half_r, chain_s, chain_r, out_s, n_s, n_r) = scratch[11 + m :]
    starts = [sum(g[0] for g in groups[:i]) for i in range(n_lhs + 1)]
    last = starts[-1]
    count = last + 1
    fc_cols = D // CHUNK
    n_held = 4 * fc_cols
    half = CHUNK // 2
    dp, z = lax.axis_index("dp"), lax.axis_index("view")
    core = dp % 2
    own = [(dp // (2 ** (m - d))) % 2 for d in range(m)]
    partner = (dp + 1 - 2 * core, z)
    peers = [(dp + (1 - 2 * own[d]) * 2 ** (m - d), z) for d in range(m)]
    outer = (z == 0) | (z == 3)
    inner = (z == 1) | (z == 2)
    to_inner = (dp, 1 + z // 3)
    to_outer = (dp, (z - 1) * 3)
    across = (dp, 3 - z)
    orders = bit_orders(m)
    full = (slice(None),) * m

    def remote(src, dst, send, recv, device):
        return pltpu.make_async_remote_copy(
            src_ref=src, dst_ref=dst, send_sem=send, recv_sem=recv, device_id=device, device_id_type=MESH
        )

    def local(src, dst, sem):
        return pltpu.make_async_copy(src, dst, sem)

    def slot(k):
        return lax.rem(k, SLOTS)

    def ring(k):
        return lax.rem(k, RING)

    def guarded(k, limit, step):
        @pl.when((k >= 0) & (k < limit))
        def _():
            step(k)

    def at_chunk(k):
        return pl.ds(pl.multiple_of(k * CHUNK, CHUNK), CHUNK)

    def lhs_load(g):
        dst = lhs.at[g % 2]
        repeats = groups[g][2]
        if repeats == 1:
            return [local(lhs_in[g], dst, lhs_s.at[g % 2])]
        return [
            local(lhs_in[g].at[i // repeats], dst.at[pl.ds(i * ROWS, ROWS)], lhs_s.at[g % 2])
            for i in range(LHS_ROWS // ROWS)
        ]

    def rhs_load(k):
        for g in range(n_lhs):

            @pl.when((k >= starts[g]) & (k < starts[g + 1]))
            def _():
                local(rhs_in[g].at[:, at_chunk(k - starts[g])], rhs.at[ring(k)], rhs_s.at[ring(k)]).start()

    local(extra_in, extra, extra_s).start()
    for g in range(2):
        for item in lhs_load(g):
            item.start()
    for k in range(RING - 1):
        rhs_load(jnp.int32(k))

    def held_load(j):
        src = fc_in.at[pl.ds(pl.multiple_of((j // fc_cols) * rows, 8), rows), at_chunk(j % fc_cols)]
        local(src, held.at[j], held_s.at[j]).start()

    def held_all(j, carry):
        held_load(j)
        return carry

    lax.fori_loop(0, n_held, held_all, 0)

    barrier = pltpu.get_barrier_semaphore()
    for peer in [partner] + peers:
        pl.semaphore_signal(barrier, inc=1, device_id=peer, device_id_type=MESH)

    @pl.when(outer)
    def _():
        pl.semaphore_signal(barrier, inc=1, device_id=to_inner, device_id_type=MESH)
        pl.semaphore_wait(barrier, m + 2)

    @pl.when(inner)
    def _():
        pl.semaphore_signal(barrier, inc=1, device_id=to_outer, device_id_type=MESH)
        pl.semaphore_signal(barrier, inc=1, device_id=across, device_id_type=MESH)
        pl.semaphore_wait(barrier, m + 3)

    def hand(k):
        src = grad.at[(ring(k),) + full + (1 - core,)]
        return remote(src, core_in.at[k], core_s.at[slot(k)], core_r.at[slot(k)], partner)

    def compute(k):
        r = ring(k)

        @pl.when(k < last)
        def _():
            group = 0
            for g in range(1, n_lhs):
                group = group + (k >= starts[g]).astype(jnp.int32)
            for g in range(n_lhs):

                @pl.when(k == starts[g])
                def _():
                    local(lhs.at[g % 2], lhs.at[g % 2], lhs_s.at[g % 2]).wait()
                    if 1 <= g < n_lhs - 1:
                        for item in lhs_load(g + 1):
                            item.start()

            local(rhs.at[r], rhs.at[r], rhs_s.at[r]).wait()
            val = dot_tn(lhs[group % 2], rhs[r])
            grad[r] = val.reshape((2,) * (m + 1) + (rows, CHUNK))

        @pl.when(k == last)
        def _():
            local(extra_in, extra, extra_s).wait()
            grad[r] = extra[...]

        @pl.when(k + RING - 1 < last)
        def _():
            rhs_load(k + RING - 1)

        hand(k).start()

    def lead(order, stage, flip):
        out = []
        for d in range(m):
            if d in order[:stage]:
                out.append(own[d])
            elif d == order[stage]:
                out.append(1 - own[d] if flip else own[d])
            else:
                out.append(slice(None))
        return tuple(out)

    def exchange(k, stage, side):
        order = orders[side]
        s = slot(k)
        cols = slice(side * half, (side + 1) * half)
        return remote(
            work.at[(k,) + lead(order, stage, True) + (slice(None), cols)],
            stage_in[stage].at[k, side],
            half_s.at[s, stage, side],
            half_r.at[s, stage, side],
            peers[order[stage]],
        )

    def by_rows(body):
        def go(i, carry):
            body(pl.ds(pl.multiple_of(i * 8, 8), 8))
            return carry

        lax.fori_loop(0, rows // 8, go, 0)

    def merge_core(k):
        hand(k).wait()

        def body(r):
            at = full + (r, slice(None))
            work[(k,) + at] = grad[(ring(k),) + full + (core, r, slice(None))] + core_in[(k,) + at]

        by_rows(body)
        for side in range(2):
            exchange(k, 0, side).start()

    def merge_stage(k, stage):
        for side in range(2):
            exchange(k, stage, side).wait()
            order = orders[side]
            cols = slice(side * half, (side + 1) * half)

            def body(r):
                at = (k,) + lead(order, stage, False) + (r, cols)
                work[at] = work[at] + stage_in[stage][(k, side) + (slice(None),) * (m - stage - 1) + (r, slice(None))]

            by_rows(body)
            if stage + 1 < m:
                exchange(k, stage + 1, side).start()
        if stage + 1 == m:

            @pl.when(outer)
            def _():
                chain(0, k, 0).start()

    def mine(track, k):
        return work.at[(k,) + tuple(own)] if track == 0 else held.at[k]

    def index(track, k):
        return k if track == 0 else count + k

    def chain(track, k, hop):
        i, s = index(track, k), slot(k)
        src = mine(track, k) if hop < 2 else za.at[i]
        dst = zb.at[i] if hop == 1 else za.at[i]
        device = (to_inner, across, to_outer)[hop]
        return remote(src, dst, chain_s.at[s, track, hop], chain_r.at[s, track, hop], device)

    def open_held(k):
        local(held.at[k], held.at[k], held_s.at[k]).wait()

        @pl.when(outer)
        def _():
            chain(1, k, 0).start()

    def meet(k, track):
        @pl.when(inner)
        def _():
            chain(track, k, 0).wait_recv()
            ref, i = mine(track, k), index(track, k)

            def body(r):
                ref[r, :] = ref[r, :] + za[i, r, :]

            by_rows(body)
            chain(track, k, 1).start()

    def total(k, track):
        @pl.when(inner)
        def _():
            chain(track, k, 1).wait()
            ref, i = mine(track, k), index(track, k)

            def body(r):
                za[i, r, :] = ref[r, :] + zb[i, r, :]

            by_rows(body)
            chain(track, k, 2).start()

    lanes = lax.broadcasted_iota(jnp.int32, (8, CHUNK), 1)

    def finish(k, track):
        i, s = index(track, k), slot(k)

        @pl.when(outer)
        def _():
            chain(track, k, 0).wait_send()
            chain(track, k, 2).wait_recv()

        @pl.when(inner)
        def _():
            chain(track, k, 2).wait_send()

        @pl.when(k >= SLOTS)
        def _():
            local(za.at[i], za.at[i], out_s.at[s, track]).wait()

        if track == 0:
            column = groups[-1][1] + groups[-1][0] + k - last
            for g in range(n_lhs):
                column = jnp.where((k >= starts[g]) & (k < starts[g + 1]), groups[g][1] + k - starts[g], column)
            column = jnp.where(k == last, wide_out.shape[1] // CHUNK - 1, column)
            local(za.at[i], wide_out.at[:, at_chunk(column)], out_s.at[s, track]).start()
            live = (lanes < 20) | (k != last)
        else:

            dst = fc_out.at[pl.ds(pl.multiple_of((k // fc_cols) * rows, 8), rows), at_chunk(k % fc_cols)]
            local(za.at[i], dst, out_s.at[s, track]).start()
            live = None

        def body(r):
            val = za[i, r, :]
            if live is not None:
                val = jnp.where(live, val, 0.0)
            acc[...] += val * val

        by_rows(body)

    acc[...] = jnp.zeros_like(acc)
    for k in range(AHEAD):
        compute(jnp.int32(k))

    def step(t, carry):
        guarded(t, count, merge_core)
        guarded(t, n_held, open_held)
        guarded(t + AHEAD, count, compute)
        for stage in range(m):
            guarded(t - LAG * (stage + 1), count, functools.partial(merge_stage, stage=stage))
        guarded(t - LAG, n_held, functools.partial(meet, track=1))
        guarded(t - LAG * (m + 1), count, functools.partial(meet, track=0))
        guarded(t - 2 * LAG, n_held, functools.partial(total, track=1))
        guarded(t - LAG * (m + 2), count, functools.partial(total, track=0))
        guarded(t - 3 * LAG, n_held, functools.partial(finish, track=1))
        guarded(t - LAG * (m + 3), count, functools.partial(finish, track=0))
        return carry

    lax.fori_loop(0, count + LAG * (m + 3), step, 0)
    for track, size in enumerate((count, n_held)):
        for k in range(size - SLOTS, size):
            local(za.at[0], za.at[0], out_s.at[k % SLOTS, track]).wait()

    nbuf[0] = acc[:, :128] + acc[:, 128:]
    for j, peer in enumerate([partner] + peers):
        copy = remote(nbuf.at[2 * j], nbuf.at[2 * j + 1], n_s.at[j], n_r.at[j], peer)
        copy.start()
        copy.wait()
        nbuf[2 * j + 2] = nbuf[2 * j] + nbuf[2 * j + 1]
    norm_out[...] = nbuf[2 * m + 2]


def reduce_all(products, extra, fc_shard, dp):
    m = dp.bit_length() - 2
    rows = D // dp
    groups, lefts, rights = [], [], []
    for left, right, column in products:
        repeats = right.shape[0] // left.shape[0]
        lefts.append(left if repeats > 1 else left.reshape(LHS_ROWS, D))
        rights.append(right.reshape(LHS_ROWS, right.shape[-1]))
        groups.append((right.shape[-1] // CHUNK, column // CHUNK, repeats))
    count = sum(g[0] for g in groups) + 1
    n_held = 4 * D // CHUNK
    width = 6 * D + FF + CHUNK
    lead = (2,) * m
    dma = pltpu.SemaphoreType.DMA
    vmem = pltpu.VMEM
    return pl.pallas_call(
        functools.partial(reduce_kernel, m, rows, groups),
        in_specs=[ANY] * (2 * len(groups) + 2),
        out_specs=[ANY, ANY, pl.BlockSpec(memory_space=pltpu.VMEM)],
        out_shape=[
            jax.ShapeDtypeStruct((rows, width), f32),
            jax.ShapeDtypeStruct((4 * rows, D), f32),
            jax.ShapeDtypeStruct((8, 128), f32),
        ],
        scratch_shapes=[
            vmem((count,) + lead + (rows, CHUNK), f32),
            vmem((count,) + lead + (rows, CHUNK), f32),
            vmem((8, CHUNK), f32),
            vmem((RING,) + lead + (2, rows, CHUNK), f32),
            vmem((2, LHS_ROWS, D), bf16),
            vmem((RING, LHS_ROWS, CHUNK), bf16),
            vmem((n_held, rows, CHUNK), f32),
            vmem(lead + (2, rows, CHUNK), f32),
        ]
        + [vmem((count, 2) + (2,) * (m - s - 1) + (rows, CHUNK // 2), f32) for s in range(m)]
        + [
            vmem((count + n_held, rows, CHUNK), f32),
            vmem((count + n_held, rows, CHUNK), f32),
            vmem((2 * m + 3, 8, 128), f32),
            dma((2,)), dma((RING,)), dma((n_held,)), dma, dma((SLOTS,)), dma((SLOTS,)),
            dma((SLOTS, m, 2)), dma((SLOTS, m, 2)), dma((SLOTS, 2, 3)), dma((SLOTS, 2, 3)), dma((SLOTS, 2)),
            dma((m + 1,)), dma((m + 1,)),
        ],
        compiler_params=pltpu.CompilerParams(
            vmem_limit_bytes=VMEM_BYTES, collective_id=0, has_side_effects=True
        ),
        cost_estimate=pl.CostEstimate(
            flops=2 * LHS_ROWS * D * CHUNK * count, bytes_accessed=60_000_000, transcendentals=0
        ),
        name="reduce_gradients",
    )(
        *lefts, *rights, extra.reshape(lead + (2, rows, CHUNK)), fc_shard
    )
def enter_gather(m):
    dp, z = lax.axis_index("dp"), lax.axis_index("view")
    core = dp % 2
    own = [(dp // (2 ** (m - d))) % 2 for d in range(m)]
    partner = (dp + 1 - 2 * core, z)
    peers = [(dp + (1 - 2 * own[d]) * 2 ** (m - d), z) for d in range(m)]
    return core, own, partner, peers


def greet_gather(m):
    _, _, partner, peers = enter_gather(m)
    barrier = pltpu.get_barrier_semaphore()
    for peer in [partner] + peers:
        pl.semaphore_signal(barrier, inc=1, device_id=peer, device_id_type=MESH)
    pl.semaphore_wait(barrier, m + 1)


def gather_steps(m, flows, ins, outs, sems):
    own_s, step_s, step_r, core_s, core_r = sems
    n_arr = len(ins)
    core, own, partner, peers = enter_gather(m)
    orders = bit_orders(m)

    def remote(src, dst, send, recv, device):
        return pltpu.make_async_remote_copy(
            src_ref=src, dst_ref=dst, send_sem=send, recv_sem=recv, device_id=device, device_id_type=MESH
        )

    def region(i, known, flip=None, which=core):
        a, lo, hi, _ = flows[i]
        lead = tuple(slice(None) if d in known else (1 - own[d] if d == flip else own[d]) for d in range(m))
        return outs[a].at[lead + (which, slice(None), pl.ds(lo, hi - lo))]

    def mine(i):
        a, lo, hi, _ = flows[i]
        return ins[a].at[:, pl.ds(lo, hi - lo)]

    def send(i, s):
        order = orders[flows[i][3]]
        src = mine(i) if s == 0 else region(i, order[:s])
        return remote(src, region(i, order[:s]), step_s.at[i, s], step_r.at[i, s], peers[order[s]])

    def arrive(i, s):
        order = orders[flows[i][3]]
        ref = region(i, order[:s], order[s])
        return remote(ref, ref, step_s.at[i, s], step_r.at[i, s], peers[order[s]])

    def hand_over(i, s):
        order = orders[flows[i][3]]
        if s == 0:
            return remote(mine(i), region(i, ()), core_s.at[i, 0], core_r.at[i, 0], partner)
        ref = region(i, order[: s - 1], order[s - 1])
        return remote(ref, ref, core_s.at[i, s], core_r.at[i, s], partner)

    def taken(i, s):
        order = orders[flows[i][3]]
        ref = region(i, (), None, 1 - core) if s == 0 else region(i, order[: s - 1], order[s - 1], 1 - core)
        return remote(ref, ref, core_s.at[i, s], core_r.at[i, s], partner)

    keeps = [
        pltpu.make_async_copy(ins[a], outs[a].at[tuple(own) + (core,)], own_s.at[a]) for a in range(n_arr)
    ]

    def begin():
        for i in range(len(flows)):
            send(i, 0).start()
        for keep in keeps:
            keep.start()
        for i in range(len(flows)):
            hand_over(i, 0).start()

    def kept():
        for keep in keeps:
            keep.wait()

    def advance(which, s):
        for i in which:
            arrive(i, s).wait_recv()
            if s + 1 < m:
                send(i, s + 1).start()
            hand_over(i, s + 1).start()

    def close():
        for i in range(len(flows)):
            for s in range(m):
                send(i, s).wait_send()
            for s in range(m + 1):
                hand_over(i, s).wait_send()
                taken(i, s).wait_recv()

    return begin, kept, advance, close


def gather_sems(n_arr, n_flows, m):
    dma = pltpu.SemaphoreType.DMA
    return [dma((n_arr,)), dma((n_flows, m)), dma((n_flows, m)), dma((n_flows, m + 1)), dma((n_flows, m + 1))]


def gather_kernel(m, flows, freqs, *refs):
    n_arr = 1 + max(a for a, _, _, _ in flows)
    ins, outs, table = refs[:n_arr], refs[n_arr : 2 * n_arr], refs[2 * n_arr]
    greet_gather(m)
    begin, kept, advance, close = gather_steps(m, flows, ins, outs, refs[2 * n_arr + 1 :])
    begin()
    odd = lax.broadcasted_iota(jnp.int32, (8, D), 1) % 2 == 1

    def fill(i, carry):
        at = i * 8 + lax.broadcasted_iota(jnp.int32, (8, D), 0)
        place = jnp.where(at < NP, at + 1, 0)
        angle = place.astype(f32) * freqs[...]
        val = jnp.where(odd, jnp.cos(angle), jnp.sin(angle))
        table[pl.ds(pl.multiple_of(i * 8, 8), 8), :] = jnp.where(at <= NP, val, 0.0)
        return carry

    lax.fori_loop(0, ROWS // 8, fill, 0)
    kept()
    for s in range(m):
        advance(range(len(flows)), s)
    close()


def gather_weights(freqs, arrays, dp):
    m = dp.bit_length() - 2
    flows = []
    for a, item in enumerate(arrays):
        cols = item.shape[1]
        if cols >= 2 * 128:
            flows += [(a, 0, cols // 2, 0), (a, cols // 2, cols, 1)]
        else:
            flows.append((a, 0, cols, 0))
    lead = (2,) * m + (2,)
    vmem = pl.BlockSpec(memory_space=pltpu.VMEM)
    count = len(flows)
    *full, table = pl.pallas_call(
        functools.partial(gather_kernel, m, flows),
        in_specs=[vmem] * (1 + len(arrays)),
        out_specs=[ANY] * len(arrays) + [vmem],
        out_shape=[jax.ShapeDtypeStruct(lead + item.shape, item.dtype) for item in arrays]
        + [jax.ShapeDtypeStruct((ROWS, D), f32)],
        scratch_shapes=gather_sems(len(arrays), count, m),
        compiler_params=pltpu.CompilerParams(
            vmem_limit_bytes=VMEM_BYTES, collective_id=1, has_side_effects=True
        ),
        cost_estimate=pl.CostEstimate(flops=1_000_000, bytes_accessed=20_000_000, transcendentals=400_000),
        name="gather_weights",
    )(freqs, *arrays)
    return [item.reshape((dp * item.shape[-2], item.shape[-1])) for item in full], table


def adam_step(grad_in, first, second, master, rate, decay, bias_one, bias_two):
    first_new = beta_one * first + (1.0 - beta_one) * grad_in
    second_new = beta_two * second + (1.0 - beta_two) * grad_in * grad_in
    ratio = first_new / bias_one / (jnp.sqrt(second_new / bias_two) + adam_eps)
    return (master - rate * (ratio + decay * master), first_new, second_new)


def update_all(grad_list, first_list, second_list, master_list, factor, bias_one, bias_two):
    rates = (rate_matrix, rate_matrix, rate_vector)
    decays = (decay_matrix, decay_matrix, 0.0)
    results = []
    for index in range(3):
        results.extend(
            adam_step(
                grad_list[index] * factor,
                first_list[index],
                second_list[index],
                master_list[index],
                rates[index],
                decays[index],
                bias_one,
                bias_two,
            )
        )
    return results


def body(
    pixels,
    patch_masks,
    teacher_wide,
    teacher_fc2,
    teacher_vec,
    student_wide,
    student_fc2,
    student_vec,
    wide_first,
    wide_second,
    fc2_first,
    fc2_second,
    vec_first,
    vec_second,
    step_count,
):
    view_id = lax.axis_index("view")
    view_count = lax.axis_size("view")
    group_size = pixels.shape[0]
    owned_images = group_size // view_count
    masked = jnp.sum(patch_masks).astype(f32)
    small = jnp.concatenate(
        [
            student_vec.astype(bf16).astype(f32),
            teacher_vec.astype(f32),
            jnp.broadcast_to(masked, (1, student_vec.shape[1])),
            jnp.zeros((128 - 41, student_vec.shape[1]), f32),
        ],
        axis=0,
    ).T
    shards = lax.axis_size("dp")
    (s_wide, s_second, tables), table = gather_weights(
        frequencies(), (student_wide.astype(bf16), student_fc2.astype(bf16), small), shards
    )
    tables = tables.T
    s_vectors, t_vectors = tables[:20], tables[20:40]
    masked_total = jnp.sum(tables[40, :: D // shards])
    divisor = masked_total * math.sqrt(D)
    own_pixels = lax.dynamic_slice_in_dim(pixels, view_id * owned_images, owned_images, 0)
    own_masks = lax.dynamic_slice_in_dim(patch_masks, view_id * owned_images, owned_images, 0)
    own_masks = own_masks.reshape(owned_images * view_count, NP)
    mask = jnp.pad(own_masks.astype(f32), ((0, 0), (0, ROWS - NP)))[:, :, None]
    (e, h, qkv, lse, o, a, h2, gp, g, f), t_wide, t_second = forward(
        False, own_pixels, mask, table, s_vectors, s_wide, s_second, (teacher_wide, teacher_fc2), shards
    )
    targets = forward(True, own_pixels, None, table, t_vectors, t_wide, t_second)
    y, dpred, df, du, dx1, acc_mlp, acc_b1 = back_mlp(
        divisor.reshape(1, 1), e, a, f, targets, mask, gp, s_vectors, s_wide, s_second
    )
    fc_shard = lax.psum_scatter(weight_grad(g, df), "dp", scatter_dimension=0, tiled=True)
    da, dqkv, dbase, acc_att = back_attention(dx1, a, e, qkv, lse, mask, s_vectors, s_wide)
    loss_part = jnp.sum(acc_mlp[0])
    g_vec = jnp.concatenate([acc_att[:9], acc_mlp[9:], acc_b1.reshape(-1, D)], axis=0)
    extra = jnp.concatenate([g_vec, jnp.broadcast_to(loss_part, (1, D)), jnp.zeros((CHUNK - 21, D), f32)], axis=0)
    steps_done = step_count[0].astype(f32)
    bias_one = 1.0 - jnp.power(beta_one, steps_done)
    bias_two = 1.0 - jnp.power(beta_two, steps_done)
    wide_all, shard_second, squares = reduce_all(
        (
            (h2, du, 5 * D),
            (y, dpred, 5 * D + FF),
            (o, da, 4 * D),
            (h, dqkv, D),
            (jnp.pad(own_pixels, ((0, 0), (0, ROWS - NP), (0, 0))), dbase, 0),
        ),
        extra.T,
        fc_shard,
        shards,
    )
    width = student_wide.shape[1]
    shard_wide, shard_vec = wide_all[:, :width], wide_all[:, width : width + 20].T
    loss_all = wide_all[0, width + 20]
    grad_list = (shard_wide, shard_second, shard_vec)
    grad_norm = jnp.sqrt(jnp.sum(squares))
    factor = jnp.minimum(1.0, clip_limit / grad_norm)
    results = update_all(
        grad_list,
        (wide_first, fc2_first, vec_first),
        (wide_second, fc2_second, vec_second),
        (student_wide, student_fc2, student_vec),
        factor,
        bias_one,
        bias_two,
    )
    return ((loss_all / divisor).reshape(1), grad_norm.reshape(1), *results)


def solution(mesh):
    in_specs = (
        P("dp", None, None),
        P("dp", None, None),
        P("dp", None),
        P("dp", None),
        P(None, "dp"),
        P("dp", None),
        P("dp", None),
        P(None, "dp"),
        P("dp", None),
        P("dp", None),
        P("dp", None),
        P("dp", None),
        P(None, "dp"),
        P(None, "dp"),
        P(),
    )
    out_specs = (
        P(),
        P(),
        P("dp", None),
        P("dp", None),
        P("dp", None),
        P("dp", None),
        P("dp", None),
        P("dp", None),
        P(None, "dp"),
        P(None, "dp"),
        P(None, "dp"),
    )
    return jax.shard_map(body, mesh=mesh, in_specs=in_specs, out_specs=out_specs, check_vma=False)
```
